128 devices in a mesh: book: 8 (over y, core), path: 16 (over z, x).
Axes of the slice: x: 4, y: 4, z: 4, core: 2. Of those that a mesh axis runs over, the one named last changes fastest.
Arguments:
- states: float32 [10, 20, 262144], P(None, None, ('book', 'path')), parts along dimension 2, may hold values from -7.5 to 7.5
- itm_flags: int32 [10, 262144], P(None, ('book', 'path')), parts along dimension 1, may hold values 0 or 1
- terminal: float32 [262144], P(('book', 'path')), parts along dimension 0, may hold values from -3.5 to 5.5
- strike: float32 [8], P('book'), parts along dimension 0, may hold values from 0.025 to 0.035
- date_index: int32 [262144], P(('book', 'path')), parts along dimension 0, may hold values from 0 to 9
Outputs:
- cash_flow: float32 [262144], P(('book', 'path')), parts along dimension 0
- book_price: float32 [8], P('book'), parts along dimension 0
- coefficients: float32 [80, 231], P('book'), parts along dimension 0
The draws below stay inside these ranges and needn't reach their ends.
There are 8 independent parts, one for each index of `book`. The reference program is written for one: setup_inputs(seed, part) draws one part's arguments, and reference() takes and returns one part's arrays. A program takes and returns all parts, laid end to end along the dimension named above; each array names one. Nothing has to cross between parts.
All inputs are finite; a program needn't handle non-finite values. No bound on the sum of `itm_flags` on one device may be relied on, other than what follows from the above.
Results may differ from the reference program's by a relative error of at most 0.0003.
Values sent between devices are 32-bit elements; how exact they have to be, the bound alone decides.
No kernel may reach another device: no remote copies, remote signals or barrier semaphores. Data moves between devices by JAX's collectives and lax.ppermute only.
A program may use at most 192 MiB of HBM per device.

```python
import jax
import jax.numpy as jnp
import numpy as np
from jax import lax

FACTORS = 20
DATES = 10
PATHS = 32768


def draw_states(key, part):
    position = (jnp.arange(PATHS, dtype=jnp.float32) + 0.5) / PATHS
    centre = 2.0 * position - 1.0
    spread = 0.5 * 3.0 ** position
    noise = jnp.clip(jax.random.normal(key, (DATES, FACTORS, PATHS), jnp.float32), -4.0, 4.0)
    offset = jnp.zeros((1, FACTORS, 1), jnp.float32)
    return centre + offset + spread * noise


def draw_terminal(key, part):
    position = (jnp.arange(PATHS, dtype=jnp.float32) + 0.5) / PATHS
    noise = jnp.clip(jax.random.normal(key, (PATHS,), jnp.float32), -4.0, 4.0)
    return 2.0 * position + 0.75 * noise


def set_ends(array, own_key, least, high):
    place = [jax.random.randint(jax.random.fold_in(own_key, axis), (), 0, length) for axis, length in enumerate(array.shape)]
    widest = array.shape.index(max(array.shape))
    beside = place[:widest] + [(place[widest] + 1) % array.shape[widest]] + place[widest + 1:]
    return array.at[tuple(place)].set(least).at[tuple(beside)].set(high)


def setup_inputs(seed: int = 0, part: int = 0) -> dict:
    key_list = jax.random.split(jax.random.key(seed), 6)
    part_splits = jax.random.split(jax.random.fold_in(key_list[5], part), 6)
    states = draw_states(jax.random.fold_in(jax.random.fold_in(key_list[5], part), 71), part)
    itm_flags = set_ends((jax.random.randint(part_splits[1], (DATES, PATHS), 0, 2) < 1).astype(jnp.int32), jax.random.fold_in(part_splits[1], 1), 0, 1)
    terminal = draw_terminal(jax.random.fold_in(jax.random.fold_in(key_list[5], part), 71), part)
    strike = jnp.clip(jax.random.uniform(part_splits[3], (1,), jnp.float32, 0.025, 0.035), 0.025, 0.035)
    date_index = set_ends(jax.random.randint(part_splits[4], (PATHS,), 0, DATES), jax.random.fold_in(part_splits[4], 1), 0, DATES - 1).astype(jnp.int32)
    return {"states": states, "itm_flags": itm_flags, "terminal": terminal, "strike": strike, "date_index": date_index}


ridge_weight = 0.05
temper_scale = 0.5
highest = lax.Precision.HIGHEST

def swap_terms(factors, strike_level):
    forwards = 0.03 * jnp.exp(0.25 * factors)
    discount = jnp.cumprod(1.0 / (1.0 + 0.25 * forwards), axis=0)
    annuity = 0.25 * lax.optimization_barrier(jnp.sum(discount, axis=0))
    swap_rate = (1.0 - discount[-1]) / annuity
    return (100.0 * annuity * (swap_rate - strike_level), discount[0])

def basis_of(scaled, pair_left, pair_right):
    ones_row = jnp.ones((1, scaled.shape[1]), scaled.dtype)
    return jnp.concatenate([ones_row, scaled, scaled[pair_left] * scaled[pair_right]], axis=0)

def solve_coefs(gram_sums, rhs_sums, path_count):
    system = gram_sums / path_count + ridge_weight * jnp.eye(gram_sums.shape[0], dtype=gram_sums.dtype)
    factor_chol = jnp.linalg.cholesky(system)
    return jax.scipy.linalg.cho_solve((factor_chol, True), rhs_sums / path_count)

def reference(states, itm_flags, terminal, strike, date_index):
    pair_left, pair_right = np.triu_indices(FACTORS)
    value_now = terminal
    coef_list = []
    for date_step in range(DATES - 1, -1, -1):
        factors = states[date_step]
        exercise, discount = swap_terms(factors, strike[0])
        value_now = value_now * discount
        money_flags = itm_flags[date_step].astype(jnp.float32)
        path_count = jnp.sum(money_flags)
        mean_vals = lax.optimization_barrier(jnp.sum(money_flags * factors, axis=1)) / path_count
        variance = lax.optimization_barrier(jnp.sum(money_flags * factors * factors, axis=1)) / path_count - mean_vals * mean_vals
        scale_vals = jnp.sqrt(variance + 1e-05)
        scaled = (factors - mean_vals[:, None]) / scale_vals[:, None]
        basis_rows = basis_of(scaled, pair_left, pair_right)
        weighted = basis_rows * money_flags
        gram_sums = lax.dot_general(weighted.astype(jnp.float32), basis_rows.astype(jnp.float32), (((1,), (1,)), ((), ())), precision=highest, preferred_element_type=jnp.float32)
        rhs_sums = jnp.dot(weighted.astype(jnp.float32), value_now.astype(jnp.float32), precision=highest, preferred_element_type=jnp.float32)
        coef_vector = solve_coefs(gram_sums, rhs_sums, path_count)
        continuation = jnp.dot(coef_vector.astype(jnp.float32), basis_rows.astype(jnp.float32), precision=highest, preferred_element_type=jnp.float32)
        open_date = (date_index <= date_step).astype(jnp.float32)
        weights = jax.nn.sigmoid((exercise - continuation) / temper_scale) * money_flags * open_date
        value_now = value_now + weights * (exercise - value_now)
        coef_list.append(coef_vector)
    book_price = jnp.reshape(jnp.sum(value_now) / PATHS, (1,))
    return (value_now, book_price, jnp.stack(coef_list[::-1], axis=0))
```

```python
import jax
import jax.numpy as jnp
from jax import lax
from jax.experimental import pallas as pl
from jax.experimental.pallas import tpu as pltpu
from jax.sharding import Mesh
from jax.sharding import PartitionSpec as P

PATH = ("path_0", "path_1")
BOOK_PATH = ("book", "path_0", "path_1")
ridge_weight = 0.05
temper_scale = 0.5
highest = lax.Precision.HIGHEST
f32 = jnp.float32
bf16 = jnp.bfloat16
NT = (((1,), (1,)), ((), ()))
TN = (((0,), (0,)), ((), ()))
ROWS = 240
HALF = 128
BLOCK = 16
CHUNK = 1024


def spec(shape, index=None):
    if index is None:
        index = (0,) * len(shape)
    return pl.BlockSpec(shape, lambda *_: index)


def lanes_of(shape):
    return lax.broadcasted_iota(jnp.int32, shape, 1)


def rows_of(shape):
    return lax.broadcasted_iota(jnp.int32, shape, 0)


def stats_kernel(z_ref, m_ref, out_ref):
    dates, factors, _ = z_ref.shape
    lane = lanes_of((factors, 128))
    packed = jnp.zeros((factors, 128), f32)
    for d in range(dates):
        z = z_ref[d]
        m = m_ref[d : d + 1, :].astype(f32)
        mz = z * m
        packed = jnp.where(lane == 3 * d, jnp.sum(mz, axis=1, keepdims=True), packed)
        packed = jnp.where(lane == 3 * d + 1, jnp.sum(mz * z, axis=1, keepdims=True), packed)
        packed = jnp.where(lane == 3 * d + 2, jnp.sum(m, axis=1, keepdims=True), packed)
    for i in range(out_ref.shape[0]):
        out_ref[i] = packed


def swap_kernel(strike_ref, z_ref, ex_ref, disc_ref, fac_ref):
    dates, factors, _ = z_ref.shape
    for d in range(dates):
        fac_ref[...] = 1.0 / (1.0 + 0.25 * (0.03 * jnp.exp(0.25 * z_ref[d])))
        first = fac_ref[0:1, :]
        disc = first
        total = first
        for j in range(1, factors):
            disc = disc * fac_ref[j : j + 1, :]
            total = total + disc
        disc_ref[d : d + 1, :] = first
        ex_ref[d : d + 1, :] = 100.0 * ((1.0 - disc) - strike_ref[0] * (0.25 * total))


def rhs_row(phi_ref, weights):
    acc = jnp.zeros((ROWS, 128), f32)
    for c in range(0, weights.shape[1], 128):
        acc = acc + phi_ref[:, c : c + 128] * weights[:, c : c + 128]
    row = lax.dot_general(
        jnp.ones((8, 128), f32), acc, NT, precision=highest, preferred_element_type=f32
    )
    return jnp.concatenate([row, jnp.zeros((8, 256 - ROWS), f32)], axis=1)


def gram_kernel(stats_ref, z_ref, m_ref, disc_ref, term_ref, phi_ref, slot_ref, v_ref, x_ref, gram_ref, rhs_ref):
    step = pl.program_id(0)
    dates = m_ref.shape[0]
    factors = z_ref.shape[0]
    paths = z_ref.shape[1]

    @pl.when(step < dates)
    def _():
        d = dates - 1 - step
        stats = stats_ref[0]
        for i in range(1, stats_ref.shape[0]):
            stats = stats + stats_ref[i]
        lane = lanes_of((factors, 128))

        def column(i):
            return jnp.sum(jnp.where(lane == i, stats, 0.0), axis=1, keepdims=True)

        count = column(3 * d + 2)
        mean = column(3 * d) / count
        inverse = 1.0 / jnp.sqrt(column(3 * d + 1) / count - mean * mean + 1e-05)
        gram_ref[...] = jnp.zeros_like(gram_ref)

        def chunk(c, carry):
            at = pl.ds(pl.multiple_of(c * CHUNK, CHUNK), CHUNK)
            x_ref[...] = (z_ref[:, at] - mean) * inverse
            phi_ref[0:1, at] = jnp.ones((1, CHUNK), f32)
            phi_ref[1 : 1 + factors, at] = x_ref[...]
            offset = 1 + factors
            for j in range(factors):
                phi_ref[offset : offset + factors - j, at] = x_ref[j : j + 1, :] * x_ref[j:factors, :]
                offset += factors - j
            phi_ref[offset:ROWS, at] = jnp.zeros((ROWS - offset, CHUNK), f32)
            phi = phi_ref[:, at]
            m = m_ref[pl.ds(d, 1), at].astype(f32)
            pad = jnp.zeros((256 - ROWS, CHUNK), bf16)
            hi = phi.astype(bf16)
            rest = phi - hi.astype(f32)
            lo = rest.astype(bf16)
            him = jnp.concatenate([(phi * m).astype(bf16), pad], axis=0)
            lom = jnp.concatenate([(rest * m).astype(bf16), pad], axis=0)
            hi = jnp.concatenate([hi, pad], axis=0)
            lo = jnp.concatenate([lo, pad], axis=0)
            gram_ref[...] += (
                lax.dot_general(him, hi, NT, preferred_element_type=f32)
                + lax.dot_general(him, lo, NT, preferred_element_type=f32)
                + lax.dot_general(lom, hi, NT, preferred_element_type=f32)
            )
            return carry

        lax.fori_loop(0, paths // CHUNK, chunk, 0)

        @pl.when(step == 0)
        def _():
            value = term_ref[...] * disc_ref[dates - 1 : dates, :]
            v_ref[...] = value
            rhs_ref[...] = rhs_row(phi_ref, value * m_ref[dates - 1 : dates, :].astype(f32))

        gram = gram_ref[...]
        slot_ref[0:HALF, :] = folded(gram[0:HALF, 0:HALF], gram[0:HALF, HALF:], gram[HALF:, HALF:])
        slot_ref[HALF:, :] = rhs_ref[...]

    @pl.when(step >= dates)
    def _():
        slot_ref[0:HALF, :] = jnp.zeros((HALF, 256), f32)
        slot_ref[HALF:, :] = rhs_ref[...]


def folded(first, beside, last):
    row, lane = rows_of((HALF, HALF)), lanes_of((HALF, HALF))
    diagonal = jnp.sum(jnp.where(row == lane, last, 0.0), axis=0, keepdims=True)
    left = jnp.where(row <= lane, first, last)
    left = jnp.where((row == HALF - 1) & (lane < HALF - 1), diagonal, left)
    return jnp.concatenate([left, beside], axis=1)


def unfolded(packed):
    row, lane = rows_of((HALF, HALF)), lanes_of((HALF, HALF))
    left, beside = packed[:, 0:HALF], packed[:, HALF:]
    turned = left.T
    first = jnp.where(row <= lane, left, turned)
    diagonal = left[HALF - 1 : HALF, :]
    last = jnp.where(row > lane, left, turned)
    last = jnp.where(row == lane, diagonal, last)
    last = jnp.where((row < HALF - 1) & (lane < HALF - 1), last, 0.0)
    return first, beside, last


def inverse_kernel(parts_ref, out_ref, a_ref):
    basis = 231
    packed = parts_ref[0, 0:HALF, :]
    for i in range(1, parts_ref.shape[0]):
        packed = packed + parts_ref[i, 0:HALF, :]
    first, beside, last = unfolded(packed)
    a_ref[0:HALF, 0:HALF] = first
    a_ref[0:HALF, HALF:] = beside
    a_ref[HALF:, 0:HALF] = beside.T
    a_ref[HALF:, HALF:] = last
    count = packed[0:1, 0:1]
    row, lane = rows_of((256, 256)), lanes_of((256, 256))
    added = jnp.where(row < basis, ridge_weight * count, 1.0)
    a_ref[...] = a_ref[...] + jnp.where(row == lane, added, 0.0)
    lane_a = lanes_of((BLOCK, 128))
    lane_b = lane_a + 128
    row_a = rows_of((BLOCK, 128))
    lane_r = lanes_of((BLOCK, 256))

    def split(x):
        one = x.astype(bf16)
        rest = x - one.astype(f32)
        two = rest.astype(bf16)
        return one, two, (rest - two.astype(f32)).astype(bf16)

    def sweep(i, carry):
        start = pl.multiple_of(i * BLOCK, BLOCK)
        panel = a_ref[pl.ds(start, BLOCK), :]
        ra, rb = panel[:, 0:128], panel[:, 128:]
        cols = []
        for c in range(BLOCK):
            both = jnp.where(lane_a == start + c, ra, 0.0) + jnp.where(lane_b == start + c, rb, 0.0)
            cols.append(jnp.broadcast_to(jnp.sum(both, axis=1, keepdims=True), (BLOCK, 128)))
        for k in range(BLOCK):
            pivot = 1.0 / cols[k][k : k + 1, :]
            here = row_a == k
            unit = jnp.where(here, 1.0, 0.0)
            ra = jnp.where(lane_a == start + k, unit, ra)
            rb = jnp.where(lane_b == start + k, unit, rb)
            row_k = ra[k : k + 1, :] * pivot
            ra = jnp.where(here, row_k, ra - cols[k] * row_k)
            row_k = rb[k : k + 1, :] * pivot
            rb = jnp.where(here, row_k, rb - cols[k] * row_k)
            for c in range(k + 1, BLOCK):
                f = cols[c][k : k + 1, :] * pivot
                cols[c] = jnp.where(here, f, cols[c] - cols[k] * f)
        inside = (lane_r >= start) & (lane_r < start + BLOCK)
        w = jnp.concatenate([ra, rb], axis=1)
        w = jnp.where(inside, -w, w)
        r1, r2, r3 = split(panel)
        w1, w2, w3 = split(w)
        left = jnp.concatenate([r1, r1, r2, r2, r1, r3], axis=0)
        right = jnp.concatenate([w1, w2, w1, w2, w3, w1], axis=0)
        change = lax.dot_general(left, right, TN, preferred_element_type=f32)
        within = (lane >= start) & (lane < start + BLOCK)
        a_ref[...] = jnp.where(within, 0.0, a_ref[...]) - change
        a_ref[pl.ds(start, BLOCK), :] = w
        return carry

    lax.fori_loop(0, ROWS // BLOCK, sweep, 0)
    result = -a_ref[...]
    packed = folded(result[0:HALF, 0:HALF], result[0:HALF, HALF:], result[HALF:, HALF:])
    for i in range(out_ref.shape[0]):
        out_ref[i] = packed


def unfold_kernel(packed_ref, out_ref):
    first, beside, last = unfolded(packed_ref[...])
    out_ref[0:HALF, 0:HALF] = first
    out_ref[0:HALF, HALF:] = beside
    out_ref[HALF:, 0:HALF] = beside.T[0 : ROWS - HALF, :]
    out_ref[HALF:, HALF:] = last[0 : ROWS - HALF, :]


def chain_kernel(date, *refs):
    parts_ref, inv_ref, phi_ref, ex_ref, m_ref, index_ref, v_ref, disc_ref = refs[:8]
    rhs = parts_ref[0, 0:1, :]
    for i in range(1, parts_ref.shape[0]):
        rhs = rhs + parts_ref[i, 0:1, :]
    product = inv_ref[...] * rhs
    coef = jnp.sum(product[:, 0:128] + product[:, 128:], axis=1, keepdims=True)
    coef = jnp.broadcast_to(coef, (ROWS, 128))
    continuation = []
    for c in range(0, v_ref.shape[1], 128):
        continuation.append(jnp.sum(coef * phi_ref[:, c : c + 128], axis=0, keepdims=True))
    continuation = jnp.concatenate(continuation, axis=1)
    exercise = ex_ref[date : date + 1, :]
    opened = jnp.where(index_ref[...] <= date, m_ref[date : date + 1, :].astype(f32), 0.0)
    weights = jax.nn.sigmoid((exercise - continuation) / temper_scale) * opened
    value = v_ref[...]
    value = value + weights * (exercise - value)
    if date:
        next_ref, out_ref, coef_ref, send_ref = refs[8:]
        value = value * disc_ref[date - 1 : date, :]
        row = rhs_row(next_ref, value * m_ref[date - 1 : date, :].astype(f32))
        for i in range(send_ref.shape[0]):
            send_ref[i] = row[0:1, :]
    else:
        out_ref, coef_ref, send_ref = refs[8:]
        total = jnp.broadcast_to(jnp.sum(value, axis=1, keepdims=True), (1, 128))
        for i in range(send_ref.shape[0]):
            send_ref[i] = total
    out_ref[...] = value
    coef_ref[...] = coef


def exchange(slots):
    return lax.all_to_all(slots, PATH, 0, 0, tiled=True)


def shards(states, itm_flags, terminal, strike, date_index):
    dates, factors, paths = states.shape
    size = lax.axis_size(PATH)
    sds = jax.ShapeDtypeStruct
    terminal = terminal.reshape(1, paths)
    date_index = date_index.reshape(1, paths)
    stats = pl.pallas_call(
        stats_kernel, out_shape=sds((size, factors, 128), f32), name="stats"
    )(states, itm_flags)
    stats = exchange(stats)
    exercise, discount = pl.pallas_call(
        swap_kernel,
        in_specs=[
            pl.BlockSpec(memory_space=pltpu.SMEM),
            pl.BlockSpec(memory_space=pltpu.VMEM),
        ],
        out_shape=[sds((dates, paths), f32), sds((dates, paths), f32)],
        scratch_shapes=[pltpu.VMEM((factors, paths), f32)],
        name="swap",
    )(strike, states)

    def date_of(i):
        return jnp.maximum(dates - 1 - i, 0)

    phi, slots, value = pl.pallas_call(
        gram_kernel,
        grid=(size,),
        in_specs=[
            spec((size, factors, 128)),
            pl.BlockSpec((None, factors, paths), lambda i: (date_of(i), 0, 0)),
            spec((dates, paths)),
            spec((dates, paths)),
            spec((1, paths)),
        ],
        out_specs=[
            pl.BlockSpec((None, ROWS, paths), lambda i: (date_of(i), 0, 0)),
            pl.BlockSpec((None, HALF + 8, 256), lambda i: (jnp.where(i < dates, date_of(i), i), 0, 0)),
            spec((1, paths)),
        ],
        out_shape=[
            sds((dates, ROWS, paths), f32),
            sds((size, HALF + 8, 256), f32),
            sds((1, paths), f32),
        ],
        scratch_shapes=[
            pltpu.VMEM((factors, CHUNK), f32),
            pltpu.VMEM((256, 256), f32),
            pltpu.VMEM((8, 256), f32),
        ],
        name="gram",
    )(stats, states, itm_flags, discount, terminal)
    slots = exchange(slots)
    inverse = pl.pallas_call(
        inverse_kernel,
        in_specs=[spec((size, HALF + 8, 256))],
        out_specs=spec((size, HALF, 256)),
        grid=(1,),
        out_shape=sds((size, HALF, 256), f32),
        scratch_shapes=[pltpu.VMEM((256, 256), f32)],
        name="inverse",
    )(slots)
    inverse = exchange(inverse)

    def unfold(first, number):
        return pl.pallas_call(
            unfold_kernel,
            grid=(number,),
            in_specs=[pl.BlockSpec((None, HALF, 256), lambda i: (first + i, 0, 0))],
            out_specs=pl.BlockSpec((None, ROWS, 256), lambda i: (i, 0, 0)),
            out_shape=sds((number, ROWS, 256), f32),
            name="unfold",
        )(inverse)

    last_inverse = unfold(dates - 1, 1)
    other_inverse = unfold(0, dates - 1)
    received = slots
    coefs = [None] * dates
    for date in range(dates - 1, -1, -1):
        is_last = date == dates - 1
        args = [received, last_inverse if is_last else other_inverse, phi, exercise, itm_flags, date_index, value, discount]
        in_specs = [
            spec((size, 8, 256), (0, HALF // 8, 0)) if is_last else spec((size, 1, 256)),
            spec((None, ROWS, 256), (0 if is_last else date, 0, 0)),
            spec((None, ROWS, paths), (date, 0, 0)),
            spec((dates, paths)),
            spec((dates, paths)),
            spec((1, paths)),
            spec((1, paths)),
            spec((dates, paths)),
        ]
        if date:
            args.append(phi)
            in_specs.append(spec((None, ROWS, paths), (date - 1, 0, 0)))
        width = 256 if date else 128

        def kernel(*refs, date=date):
            chain_kernel(date, *refs)

        value, coefs[date], send = pl.pallas_call(
            kernel,
            grid=(1,),
            in_specs=in_specs,
            out_specs=[spec((1, paths)), spec((ROWS, 128)), spec((size, 1, width))],
            out_shape=[sds((1, paths), f32), sds((ROWS, 128), f32), sds((size, 1, width), f32)],
            name="chain",
        )(*args)
        received = exchange(send)
    book_price = jnp.sum(received[:, 0, 0:1], axis=0) / (paths * size)
    basis = 1 + factors + factors * (factors + 1) // 2
    coefficients = jnp.stack([c[0:basis, 0] for c in coefs], axis=0)
    return (value.reshape(paths), book_price, coefficients)


def solution(mesh):
    split = Mesh(mesh.devices.reshape(mesh.shape["book"], 4, 4), ("book", "path_0", "path_1"))
    return jax.shard_map(
        shards,
        mesh=split,
        in_specs=(
            P(None, None, BOOK_PATH),
            P(None, BOOK_PATH),
            P(BOOK_PATH),
            P("book"),
            P(BOOK_PATH),
        ),
        out_specs=(P(BOOK_PATH), P("book"), P("book", None)),
        check_vma=False,
    )
```

```python
import jax
import jax.numpy as jnp
from jax import lax
from jax.experimental import pallas as pl
from jax.experimental.pallas import tpu as pltpu
from jax.sharding import Mesh
from jax.sharding import PartitionSpec as P

PATH = ("path_0", "path_1")
BOOK_PATH = ("book", "path_0", "path_1")
ridge_weight = 0.05
temper_scale = 0.5
highest = lax.Precision.HIGHEST
f32 = jnp.float32
bf16 = jnp.bfloat16
NT = (((1,), (1,)), ((), ()))
TN = (((0,), (0,)), ((), ()))
ROWS = 240
HALF = 128
BLOCK = 16
CHUNK = 1024


def spec(shape, index=None):
    if index is None:
        index = (0,) * len(shape)
    return pl.BlockSpec(shape, lambda *_: index)


WHOLE = pl.BlockSpec(memory_space=pltpu.VMEM)


def near(x):
    return pltpu.with_memory_space_constraint(x, pltpu.VMEM)


def lanes_of(shape):
    return lax.broadcasted_iota(jnp.int32, shape, 1)


def rows_of(shape):
    return lax.broadcasted_iota(jnp.int32, shape, 0)


def stats_kernel(z_ref, m_ref, out_ref):
    dates, factors, _ = z_ref.shape
    lane = lanes_of((factors, 128))
    packed = jnp.zeros((factors, 128), f32)
    for d in range(dates):
        z = z_ref[d]
        m = m_ref[d : d + 1, :].astype(f32)
        mz = z * m
        packed = jnp.where(lane == 3 * d, jnp.sum(mz, axis=1, keepdims=True), packed)
        packed = jnp.where(lane == 3 * d + 1, jnp.sum(mz * z, axis=1, keepdims=True), packed)
        packed = jnp.where(lane == 3 * d + 2, jnp.sum(m, axis=1, keepdims=True), packed)
    for i in range(out_ref.shape[0]):
        out_ref[i] = packed


def swap_kernel(strike_ref, z_ref, ex_ref, disc_ref, fac_ref):
    dates, factors, _ = z_ref.shape
    for d in range(dates):
        fac_ref[...] = 1.0 / (1.0 + 0.25 * (0.03 * jnp.exp(0.25 * z_ref[d])))
        first = fac_ref[0:1, :]
        disc = first
        total = first
        for j in range(1, factors):
            disc = disc * fac_ref[j : j + 1, :]
            total = total + disc
        disc_ref[d : d + 1, :] = first
        ex_ref[d : d + 1, :] = 100.0 * ((1.0 - disc) - strike_ref[0] * (0.25 * total))


def rhs_row(phi_ref, weights):
    acc = jnp.zeros((ROWS, 128), f32)
    for c in range(0, weights.shape[1], 128):
        acc = acc + phi_ref[:, c : c + 128] * weights[:, c : c + 128]
    row = lax.dot_general(
        jnp.ones((8, 128), f32), acc, NT, precision=highest, preferred_element_type=f32
    )
    return jnp.concatenate([row, jnp.zeros((8, 256 - ROWS), f32)], axis=1)


def gram_kernel(stats_ref, z_all_ref, m_ref, disc_ref, term_ref, *refs):
    *phi_refs, slot_ref, v_ref, phi_two_ref, x_ref, gram_ref, rhs_ref, sems = refs
    step = pl.program_id(0)
    dates, factors, paths = z_all_ref.shape
    z_ref = z_all_ref.at[jnp.maximum(dates - 1 - step, 0)]
    side = step % 2
    phi_ref = phi_two_ref.at[side]

    def copy_of(date):
        return pltpu.make_async_copy(phi_ref, phi_refs[date], sems.at[side])

    @pl.when((step >= 2) & (step < dates + 2))
    def _():
        copy_of(0).wait()

    @pl.when(step < dates)
    def _():
        d = dates - 1 - step
        stats = stats_ref[0]
        for i in range(1, stats_ref.shape[0]):
            stats = stats + stats_ref[i]
        lane = lanes_of((factors, 128))

        def column(i):
            return jnp.sum(jnp.where(lane == i, stats, 0.0), axis=1, keepdims=True)

        count = column(3 * d + 2)
        mean = column(3 * d) / count
        inverse = 1.0 / jnp.sqrt(column(3 * d + 1) / count - mean * mean + 1e-05)
        gram_ref[...] = jnp.zeros_like(gram_ref)

        def chunk(c, carry):
            at = pl.ds(pl.multiple_of(c * CHUNK, CHUNK), CHUNK)
            x_ref[...] = (z_ref[:, at] - mean) * inverse
            phi_ref[0:1, at] = jnp.ones((1, CHUNK), f32)
            phi_ref[1 : 1 + factors, at] = x_ref[...]
            offset = 1 + factors
            for j in range(factors):
                phi_ref[offset : offset + factors - j, at] = x_ref[j : j + 1, :] * x_ref[j:factors, :]
                offset += factors - j
            phi_ref[offset:ROWS, at] = jnp.zeros((ROWS - offset, CHUNK), f32)
            phi = phi_ref[:, at]
            m = m_ref[pl.ds(d, 1), at].astype(f32)
            pad = jnp.zeros((256 - ROWS, CHUNK), bf16)
            hi = phi.astype(bf16)
            rest = phi - hi.astype(f32)
            lo = rest.astype(bf16)
            him = jnp.concatenate([(phi * m).astype(bf16), pad], axis=0)
            lom = jnp.concatenate([(rest * m).astype(bf16), pad], axis=0)
            hi = jnp.concatenate([hi, pad], axis=0)
            lo = jnp.concatenate([lo, pad], axis=0)
            gram_ref[...] += (
                lax.dot_general(him, hi, NT, preferred_element_type=f32)
                + lax.dot_general(him, lo, NT, preferred_element_type=f32)
                + lax.dot_general(lom, hi, NT, preferred_element_type=f32)
            )
            return carry

        lax.fori_loop(0, paths // CHUNK, chunk, 0)
        for date in range(dates):

            @pl.when(d == date)
            def _(date=date):
                copy_of(date).start()

        @pl.when(step == 0)
        def _():
            value = term_ref[...] * disc_ref[dates - 1 : dates, :]
            v_ref[...] = value
            rhs_ref[...] = rhs_row(phi_ref, value * m_ref[dates - 1 : dates, :].astype(f32))

        gram = gram_ref[...]
        slot_ref[0:HALF, :] = folded(gram[0:HALF, 0:HALF], gram[0:HALF, HALF:], gram[HALF:, HALF:])
        slot_ref[HALF:, :] = rhs_ref[...]

    @pl.when(step >= dates)
    def _():
        slot_ref[0:HALF, :] = jnp.zeros((HALF, 256), f32)
        slot_ref[HALF:, :] = rhs_ref[...]


def folded(first, beside, last):
    row, lane = rows_of((HALF, HALF)), lanes_of((HALF, HALF))
    diagonal = jnp.sum(jnp.where(row == lane, last, 0.0), axis=0, keepdims=True)
    left = jnp.where(row <= lane, first, last)
    left = jnp.where((row == HALF - 1) & (lane < HALF - 1), diagonal, left)
    return jnp.concatenate([left, beside], axis=1)


def unfolded(packed):
    row, lane = rows_of((HALF, HALF)), lanes_of((HALF, HALF))
    left, beside = packed[:, 0:HALF], packed[:, HALF:]
    turned = left.T
    first = jnp.where(row <= lane, left, turned)
    diagonal = left[HALF - 1 : HALF, :]
    last = jnp.where(row > lane, left, turned)
    last = jnp.where(row == lane, diagonal, last)
    last = jnp.where((row < HALF - 1) & (lane < HALF - 1), last, 0.0)
    return first, beside, last


def inverse_kernel(parts_ref, out_ref, a_ref):
    basis = 231
    packed = parts_ref[0, 0:HALF, :]
    for i in range(1, parts_ref.shape[0]):
        packed = packed + parts_ref[i, 0:HALF, :]
    first, beside, last = unfolded(packed)
    a_ref[0:HALF, 0:HALF] = first
    a_ref[0:HALF, HALF:] = beside
    a_ref[HALF:, 0:HALF] = beside.T
    a_ref[HALF:, HALF:] = last
    count = packed[0:1, 0:1]
    row, lane = rows_of((256, 256)), lanes_of((256, 256))
    added = jnp.where(row < basis, ridge_weight * count, 1.0)
    a_ref[...] = a_ref[...] + jnp.where(row == lane, added, 0.0)
    lane_a = lanes_of((BLOCK, 128))
    lane_b = lane_a + 128
    row_a = rows_of((BLOCK, 128))
    lane_r = lanes_of((BLOCK, 256))

    def split(x):
        one = x.astype(bf16)
        rest = x - one.astype(f32)
        two = rest.astype(bf16)
        return one, two, (rest - two.astype(f32)).astype(bf16)

    def sweep(i, carry):
        start = pl.multiple_of(i * BLOCK, BLOCK)
        panel = a_ref[pl.ds(start, BLOCK), :]
        ra, rb = panel[:, 0:128], panel[:, 128:]
        cols = []
        for c in range(BLOCK):
            both = jnp.where(lane_a == start + c, ra, 0.0) + jnp.where(lane_b == start + c, rb, 0.0)
            cols.append(jnp.broadcast_to(jnp.sum(both, axis=1, keepdims=True), (BLOCK, 128)))
        for k in range(BLOCK):
            pivot = 1.0 / cols[k][k : k + 1, :]
            here = row_a == k
            unit = jnp.where(here, 1.0, 0.0)
            ra = jnp.where(lane_a == start + k, unit, ra)
            rb = jnp.where(lane_b == start + k, unit, rb)
            row_k = ra[k : k + 1, :] * pivot
            ra = jnp.where(here, row_k, ra - cols[k] * row_k)
            row_k = rb[k : k + 1, :] * pivot
            rb = jnp.where(here, row_k, rb - cols[k] * row_k)
            for c in range(k + 1, BLOCK):
                f = cols[c][k : k + 1, :] * pivot
                cols[c] = jnp.where(here, f, cols[c] - cols[k] * f)
        inside = (lane_r >= start) & (lane_r < start + BLOCK)
        w = jnp.concatenate([ra, rb], axis=1)
        w = jnp.where(inside, -w, w)
        r1, r2, r3 = split(panel)
        w1, w2, w3 = split(w)
        left = jnp.concatenate([r1, r1, r2, r2, r1, r3], axis=0)
        right = jnp.concatenate([w1, w2, w1, w2, w3, w1], axis=0)
        change = lax.dot_general(left, right, TN, preferred_element_type=f32)
        within = (lane >= start) & (lane < start + BLOCK)
        a_ref[...] = jnp.where(within, 0.0, a_ref[...]) - change
        a_ref[pl.ds(start, BLOCK), :] = w
        return carry

    lax.fori_loop(0, ROWS // BLOCK, sweep, 0)
    result = -a_ref[...]
    packed = folded(result[0:HALF, 0:HALF], result[0:HALF, HALF:], result[HALF:, HALF:])
    for i in range(out_ref.shape[0]):
        out_ref[i] = packed


def unfold_kernel(packed_ref, out_ref):
    for i in range(out_ref.shape[0]):
        first, beside, last = unfolded(packed_ref[i])
        out_ref[i, 0:HALF, 0:HALF] = first
        out_ref[i, 0:HALF, HALF:] = beside
        out_ref[i, HALF:, 0:HALF] = beside.T[0 : ROWS - HALF, :]
        out_ref[i, HALF:, HALF:] = last[0 : ROWS - HALF, :]


def chain_kernel(date, dates, *refs):
    inv_ref, parts_ref, phi_ref, ex_ref, m_ref, index_ref, v_ref, disc_ref = refs[:8]
    refs = refs[8:]
    if date:
        next_ref = refs[0]
        refs = refs[1:]
    if date == dates - 1:
        coefs = jnp.zeros((ROWS, 128), f32)
    else:
        coefs = refs[0][...]
        refs = refs[1:]
    rhs = parts_ref[0, 0:1, :]
    for i in range(1, parts_ref.shape[0]):
        rhs = rhs + parts_ref[i, 0:1, :]
    product = inv_ref[date] * rhs
    coef = jnp.sum(product[:, 0:128] + product[:, 128:], axis=1, keepdims=True)
    coef = jnp.broadcast_to(coef, (ROWS, 128))
    out_ref, coef_ref, send_ref = refs
    continuation = []
    for c in range(0, v_ref.shape[1], 128):
        continuation.append(jnp.sum(coef * phi_ref[:, c : c + 128], axis=0, keepdims=True))
    continuation = jnp.concatenate(continuation, axis=1)
    exercise = ex_ref[date : date + 1, :]
    opened = jnp.where(index_ref[...] <= date, m_ref[date : date + 1, :].astype(f32), 0.0)
    weights = jax.nn.sigmoid((exercise - continuation) / temper_scale) * opened
    value = v_ref[...]
    value = value + weights * (exercise - value)
    if date:
        value = value * disc_ref[date - 1 : date, :]
        row = rhs_row(next_ref, value * m_ref[date - 1 : date, :].astype(f32))
        for i in range(send_ref.shape[0]):
            send_ref[i] = row[0:1, :]
    else:
        total = jnp.broadcast_to(jnp.sum(value, axis=1, keepdims=True), (1, 128))
        for i in range(send_ref.shape[0]):
            send_ref[i] = total
    out_ref[...] = value
    coefs = jnp.where(lanes_of((ROWS, 128)) == date, coef, coefs)
    if date:
        coef_ref[...] = coefs
    else:
        for c in range(0, ROWS, 128):
            coef_ref[:, c : c + 128] = coefs[0:128, :].T if c == 0 else jnp.concatenate(
                [coefs[c:, :], jnp.zeros((128 - (ROWS - c), 128), f32)], axis=0
            ).T


def exchange(slots):
    return lax.all_to_all(slots, PATH, 0, 0, tiled=True)


def shards(states, itm_flags, terminal, strike, date_index):
    dates, factors, paths = states.shape
    size = lax.axis_size(PATH)
    sds = jax.ShapeDtypeStruct
    terminal = terminal.reshape(1, paths)
    date_index = date_index.reshape(1, paths)
    vmem = pltpu.VMEM
    limit = pltpu.CompilerParams(vmem_limit_bytes=24 << 20)
    stats = pl.pallas_call(
        stats_kernel,
        out_shape=vmem((size, factors, 128), f32),
        out_specs=WHOLE,
        compiler_params=limit,
        name="stats",
    )(states, itm_flags)
    stats = exchange(stats)
    exercise, discount = pl.pallas_call(
        swap_kernel,
        in_specs=[pl.BlockSpec(memory_space=pltpu.SMEM), WHOLE],
        out_specs=[WHOLE, WHOLE],
        out_shape=[vmem((dates, paths), f32), vmem((dates, paths), f32)],
        scratch_shapes=[pltpu.VMEM((factors, paths), f32)],
        compiler_params=limit,
        name="swap",
    )(strike, states)

    *phi, slots, value = pl.pallas_call(
        gram_kernel,
        grid=(size,),
        in_specs=[WHOLE, WHOLE, WHOLE, WHOLE, WHOLE],
        out_specs=[pl.BlockSpec(memory_space=pltpu.HBM)] * dates
        + [
            pl.BlockSpec((None, HALF + 8, 256), lambda i: (jnp.where(i < dates, jnp.maximum(dates - 1 - i, 0), i), 0, 0)),
            WHOLE,
        ],
        out_shape=[pltpu.HBM((ROWS, paths), f32)] * dates
        + [
            sds((size, HALF + 8, 256), f32),
            vmem((1, paths), f32),
        ],
        scratch_shapes=[
            pltpu.VMEM((2, ROWS, paths), f32),
            pltpu.VMEM((factors, CHUNK), f32),
            pltpu.VMEM((256, 256), f32),
            pltpu.VMEM((8, 256), f32),
            pltpu.SemaphoreType.DMA((2,)),
        ],
        compiler_params=limit,
        name="gram",
    )(near(stats), states, itm_flags, near(discount), terminal)
    slots = exchange(slots)
    inverse = pl.pallas_call(
        inverse_kernel,
        grid=(1,),
        in_specs=[spec((size, HALF + 8, 256))],
        out_specs=spec((size, HALF, 256)),
        out_shape=pltpu.HBM((size, HALF, 256), f32),
        scratch_shapes=[pltpu.VMEM((256, 256), f32)],
        compiler_params=limit,
        name="inverse",
    )(slots)
    inverse = exchange(inverse)
    inverse = pl.pallas_call(
        unfold_kernel,
        grid=(1,),
        in_specs=[spec((dates, HALF, 256))],
        out_specs=WHOLE,
        out_shape=vmem((dates, ROWS, 256), f32),
        compiler_params=limit,
        name="unfold",
    )(inverse)
    received = slots[:, HALF : HALF + 1, :]
    coefs = None
    for date in range(dates - 1, -1, -1):
        args = [inverse, received, phi[date], exercise, itm_flags, date_index, value, discount]
        if date:
            args.append(phi[date - 1])
        if date < dates - 1:
            args.append(coefs)

        def kernel(*refs, date=date):
            chain_kernel(date, dates, *refs)

        value, coefs, send = pl.pallas_call(
            kernel,
            in_specs=[WHOLE] * len(args),
            out_specs=[WHOLE] * 3,
            out_shape=[
                vmem((1, paths), f32),
                vmem((ROWS, 128), f32),
                vmem((size, 1, 256), f32),
            ]
            if date
            else [sds((1, paths), f32), sds((128, 256), f32), sds((size, 1, 128), f32)],
            compiler_params=limit,
            name="chain",
        )(*(near(x) for x in args))
        received = exchange(send)
    book_price = jnp.sum(received[:, 0, 0:1], axis=0) / (paths * size)
    basis = 1 + factors + factors * (factors + 1) // 2
    coefficients = coefs[0:dates, 0:basis]
    return (value.reshape(paths), book_price, coefficients)


def solution(mesh):
    split = Mesh(mesh.devices.reshape(mesh.shape["book"], 4, 4), ("book", "path_0", "path_1"))
    return jax.shard_map(
        shards,
        mesh=split,
        in_specs=(
            P(None, None, BOOK_PATH),
            P(None, BOOK_PATH),
            P(BOOK_PATH),
            P("book"),
            P(BOOK_PATH),
        ),
        out_specs=(P(BOOK_PATH), P("book"), P("book", None)),
        check_vma=False,
    )
```

```python
import jax
import jax.numpy as jnp
from jax import lax
from jax.experimental import pallas as pl
from jax.experimental.pallas import tpu as pltpu
from jax.sharding import Mesh
from jax.sharding import PartitionSpec as P

PATH = ("path_0", "path_1")
BOOK_PATH = ("book", "path_0", "path_1")
ridge_weight = 0.05
temper_scale = 0.5
highest = lax.Precision.HIGHEST
f32 = jnp.float32
bf16 = jnp.bfloat16
NT = (((1,), (1,)), ((), ()))
TN = (((0,), (0,)), ((), ()))
ROWS = 240
HALF = 128
REST = 104
SLOT = 112
BLOCK = 16
CHUNK = 1024


def spec(shape, index=None):
    if index is None:
        index = (0,) * len(shape)
    return pl.BlockSpec(shape, lambda *_: index)


WHOLE = pl.BlockSpec(memory_space=pltpu.VMEM)


def near(x):
    return pltpu.with_memory_space_constraint(x, pltpu.VMEM)


def lanes_of(shape):
    return lax.broadcasted_iota(jnp.int32, shape, 1)


def rows_of(shape):
    return lax.broadcasted_iota(jnp.int32, shape, 0)


def stats_kernel(z_ref, m_ref, out_ref):
    dates, factors, _ = z_ref.shape
    lane = lanes_of((factors, 128))
    packed = jnp.zeros((factors, 128), f32)
    for d in range(dates):
        z = z_ref[d]
        m = m_ref[d : d + 1, :].astype(f32)
        mz = z * m
        packed = jnp.where(lane == 3 * d, jnp.sum(mz, axis=1, keepdims=True), packed)
        packed = jnp.where(lane == 3 * d + 1, jnp.sum(mz * z, axis=1, keepdims=True), packed)
        packed = jnp.where(lane == 3 * d + 2, jnp.sum(m, axis=1, keepdims=True), packed)
    for i in range(out_ref.shape[0]):
        out_ref[i] = packed


def swap_kernel(strike_ref, z_ref, ex_ref, disc_ref, fac_ref):
    dates, factors, _ = z_ref.shape
    for d in range(dates):
        fac_ref[...] = 1.0 / (1.0 + 0.25 * (0.03 * jnp.exp(0.25 * z_ref[d])))
        first = fac_ref[0:1, :]
        disc = first
        total = first
        for j in range(1, factors):
            disc = disc * fac_ref[j : j + 1, :]
            total = total + disc
        disc_ref[d : d + 1, :] = first
        ex_ref[d : d + 1, :] = 100.0 * ((1.0 - disc) - strike_ref[0] * (0.25 * total))


def rhs_row(phi_ref, weights):
    acc = jnp.zeros((ROWS, 128), f32)
    for c in range(0, weights.shape[1], 128):
        acc = acc + phi_ref[c // 128] * weights[:, c : c + 128]
    row = lax.dot_general(
        jnp.ones((8, 128), f32), acc, NT, precision=highest, preferred_element_type=f32
    )
    return jnp.concatenate([row, jnp.zeros((8, 256 - ROWS), f32)], axis=1)


def column(stats, i):
    return jnp.sum(jnp.where(lanes_of(stats.shape) == i, stats, 0.0), axis=1, keepdims=True)


def moments(stats_ref, d):
    stats = stats_ref[0]
    for i in range(1, stats_ref.shape[0]):
        stats = stats + stats_ref[i]
    count = column(stats, 3 * d + 2)
    mean = column(stats, 3 * d) / count
    return mean, 1.0 / jnp.sqrt(column(stats, 3 * d + 1) / count - mean * mean + 1e-05)


def fill_basis(phi_ref, x_ref, z, m, mean, inverse):
    factors = z.shape[0]
    x_ref[0:factors, :] = (z - mean) * inverse * m
    phi_ref[0:1, :] = m
    phi_ref[1 : 1 + factors, :] = x_ref[0:factors, :]
    offset = 1 + factors
    for j in range(factors):
        left = jnp.broadcast_to(x_ref[j : j + 1, :], (8, 128))
        for k in range(0, factors - j, 8):
            phi_ref[offset + k : offset + k + 8, :] = left * x_ref[j + k : j + k + 8, :]
        offset += factors - j
    phi_ref[offset : offset + 8, :] = jnp.zeros((8, 128), f32)
    phi_ref[ROWS - 8 : ROWS, :] = jnp.zeros((8, 128), f32)


def basis_kernel(stats_ref, z_ref, m_ref, *refs):
    *phi_refs, phi_two_ref, x_ref, sems = refs
    step = pl.program_id(0)
    dates, paths = m_ref.shape
    d = dates - 1 - step
    side = step % 2

    def copy_of(half, date):
        return pltpu.make_async_copy(phi_two_ref.at[half], phi_refs[date], sems.at[half])

    @pl.when(step >= 2)
    def _():
        copy_of(side, 0).wait()

    mean, inverse = moments(stats_ref, d)
    m = m_ref[pl.ds(d, 1), :].astype(f32)
    for t in range(paths // 128):
        at = slice(t * 128, (t + 1) * 128)
        fill_basis(phi_two_ref.at[side, t], x_ref.at[t], z_ref[:, at], m[:, at], mean, inverse)
    for date in range(dates):

        @pl.when(d == date)
        def _(date=date):
            copy_of(side, date).start()

    @pl.when(step == dates - 1)
    def _():
        for half in range(2):
            copy_of(half, 0).wait()


def gram_kernel(stats_ref, z_all_ref, m_ref, disc_ref, term_ref, slots_ref, v_ref, phi_ref, x_ref, gram_ref, rhs_ref):
    step = pl.program_id(0)
    dates, factors, paths = z_all_ref.shape
    d = dates - 1 - step

    @pl.when(step == 0)
    def _():
        for t in range(phi_ref.shape[0]):
            x_ref[t] = jnp.zeros((32, 128), f32)
        v_ref[...] = term_ref[...] * disc_ref[dates - 1 : dates, :]

    mean, inverse = moments(stats_ref, d)
    gram_ref[...] = jnp.zeros_like(gram_ref)

    def chunk(c, carry):
        total = None
        span = pl.ds(pl.multiple_of(c * CHUNK, CHUNK), CHUNK)
        flags = m_ref[pl.ds(d, 1), span].astype(f32)
        values = jnp.where(step == 0, v_ref[:, span], 0.0)
        for pair in range(0, CHUNK // 128, 2):
            hi, lo = [], []
            for t in (pair, pair + 1):
                at = pl.ds(pl.multiple_of(c * CHUNK + t * 128, 128), 128)
                own = slice(t * 128, (t + 1) * 128)
                fill_basis(phi_ref.at[t], x_ref.at[t], z_all_ref[d, :, at], flags[:, own], mean, inverse)
                phi = phi_ref[t]
                high = phi.astype(bf16)
                low = (phi - high.astype(f32)).astype(bf16)
                value = values[:, own]
                one = value.astype(bf16).astype(f32)
                two = (value - one).astype(bf16).astype(f32)
                three = value - one - two
                row = rows_of((256 - ROWS, 128))
                under = jnp.where(row == 0, one, jnp.where(row == 1, two, jnp.where(row == 2, three, 0.0)))
                hi.append(jnp.concatenate([high, under.astype(bf16)], axis=0))
                lo.append(jnp.concatenate([low, jnp.zeros((256 - ROWS, 128), bf16)], axis=0))
            hi = jnp.concatenate(hi, axis=1)
            lo = jnp.concatenate(lo, axis=1)
            both = lax.dot_general(
                jnp.concatenate([hi, lo], axis=0), hi, NT, preferred_element_type=f32
            )
            part = both[0:256] + both[256:] + lax.dot_general(hi, lo, NT, preferred_element_type=f32)
            total = part if total is None else total + part
        gram_ref[...] += total
        return carry

    lax.fori_loop(0, paths // CHUNK, chunk, 0)
    gram = gram_ref[...]
    row, lane = rows_of((HALF, HALF)), lanes_of((HALF, HALF))
    beside = jnp.where(lane < REST, gram[0:HALF, HALF:], 0.0)
    under = jnp.where((row < REST) & (lane < REST), gram[HALF:, HALF:], 0.0)
    rhs = jnp.where(step == 0, jnp.sum(gram[ROWS : ROWS + 3, :], axis=0, keepdims=True), rhs_ref[...])
    rhs_ref[...] = rhs
    packed = folded(gram[0:HALF, 0:HALF], beside, under, rhs)
    slots_ref[d] = packed

    @pl.when(step == 0)
    def _():
        for i in range(dates, slots_ref.shape[0]):
            slots_ref[i] = packed


def folded(first, beside, last, rhs=None):
    row, lane = rows_of((HALF, HALF)), lanes_of((HALF, HALF))
    left = jnp.where(row <= lane, first, last)
    low_lane = lanes_of((8, HALF))
    low = left[REST:SLOT]
    low = jnp.where(low_lane < 16, pltpu.roll(first[SLOT : SLOT + 8], 16, 1), low)
    low = jnp.where((low_lane >= 16) & (low_lane < 32), pltpu.roll(first[SLOT + 8 :], 32, 1), low)
    if rhs is not None:
        low_row = rows_of((8, HALF))
        for i in range(4):
            piece = pltpu.roll(jnp.broadcast_to(rhs, (8, 256)), (32 - 72 * i) % 256, 1)[:, 0:HALF]
            low = jnp.where((low_row == i) & (low_lane >= 32) & (low_lane < REST), piece, low)
    left = jnp.concatenate([left[0:REST], low], axis=0)
    diagonal = jnp.sum(jnp.where(row == lane, last, 0.0), axis=1, keepdims=True)
    right = jnp.where(lane < REST, beside, pltpu.roll(beside.T, HALF - 8, 1))
    right = jnp.where(lane == 120, diagonal, right)[0:SLOT]
    return jnp.concatenate([left, right], axis=1)


def unfolded(packed):
    row, lane = rows_of((HALF, HALF)), lanes_of((HALF, HALF))
    none = jnp.zeros((HALF - SLOT, HALF), f32)
    left = jnp.concatenate([packed[:, 0:HALF], none], axis=0)
    right = jnp.concatenate([packed[:, HALF:], none], axis=0)
    low = left[REST:SLOT]
    corner = jnp.concatenate(
        [left[0:SLOT], pltpu.roll(low, HALF - 16, 1), pltpu.roll(low, HALF - 32, 1)], axis=0
    )
    turned = left.T
    first = jnp.where(row <= lane, left, turned)
    first = jnp.where((row >= SLOT) & (lane >= SLOT), corner, first)
    diagonal = jnp.sum(jnp.where(lane == 120, right, 0.0), axis=1, keepdims=True)
    last = jnp.where(row > lane, left, turned)
    last = jnp.where(row == lane, diagonal, last)
    last = jnp.where((row < REST) & (lane < REST), last, 0.0)
    beside = jnp.where(row < SLOT, right, pltpu.roll(right, 8, 1).T)
    beside = jnp.where(lane < REST, beside, 0.0)
    return first, beside, last


def unfolded_row(low):
    lane = lanes_of((1, 256))
    wide = jnp.concatenate([low, jnp.zeros((8, HALF), f32)], axis=1)
    total = jnp.zeros((1, 256), f32)
    for i in range(4):
        piece = pltpu.roll(wide, (72 * i - 32) % 256, 1)[i : i + 1]
        total = jnp.where((lane >= 72 * i) & (lane < min(72 * i + 72, 231)), piece, total)
    return total


def inverse_kernel(parts_ref, out_ref, a_ref):
    basis = 231
    packed = parts_ref[0]
    for i in range(1, parts_ref.shape[0]):
        packed = packed + parts_ref[i]
    first, beside, last = unfolded(packed)
    a_ref[0:HALF, 0:HALF] = first
    a_ref[0:HALF, HALF:] = beside
    a_ref[HALF:, 0:HALF] = beside.T
    a_ref[HALF:, HALF:] = last
    count = packed[0:1, 0:1]
    row, lane = rows_of((256, 256)), lanes_of((256, 256))
    added = jnp.where(row < basis, ridge_weight * count, 1.0)
    a_ref[...] = a_ref[...] + jnp.where(row == lane, added, 0.0)
    lane_a = lanes_of((BLOCK, 128))
    lane_b = lane_a + 128
    row_a = rows_of((BLOCK, 128))
    lane_r = lanes_of((BLOCK, 256))

    def split(x):
        one = x.astype(bf16)
        rest = x - one.astype(f32)
        two = rest.astype(bf16)
        return one, two, (rest - two.astype(f32)).astype(bf16)

    def sweep(i, carry):
        start = pl.multiple_of(i * BLOCK, BLOCK)
        panel = a_ref[pl.ds(start, BLOCK), :]
        ra, rb = panel[:, 0:128], panel[:, 128:]
        cols = []
        for c in range(BLOCK):
            both = jnp.where(lane_a == start + c, ra, 0.0) + jnp.where(lane_b == start + c, rb, 0.0)
            cols.append(jnp.broadcast_to(jnp.sum(both, axis=1, keepdims=True), (BLOCK, 128)))
        for k in range(BLOCK):
            pivot = 1.0 / cols[k][k : k + 1, :]
            here = row_a == k
            unit = jnp.where(here, 1.0, 0.0)
            ra = jnp.where(lane_a == start + k, unit, ra)
            rb = jnp.where(lane_b == start + k, unit, rb)
            row_k = ra[k : k + 1, :] * pivot
            ra = jnp.where(here, row_k, ra - cols[k] * row_k)
            row_k = rb[k : k + 1, :] * pivot
            rb = jnp.where(here, row_k, rb - cols[k] * row_k)
            for c in range(k + 1, BLOCK):
                f = cols[c][k : k + 1, :] * pivot
                cols[c] = jnp.where(here, f, cols[c] - cols[k] * f)
        inside = (lane_r >= start) & (lane_r < start + BLOCK)
        w = jnp.concatenate([ra, rb], axis=1)
        w = jnp.where(inside, -w, w)
        r1, r2, r3 = split(panel)
        w1, w2, w3 = split(w)
        left = jnp.concatenate([r1, r1, r2, r2, r1, r3], axis=0)
        right = jnp.concatenate([w1, w2, w1, w2, w3, w1], axis=0)
        change = lax.dot_general(left, right, TN, preferred_element_type=f32)
        within = (lane >= start) & (lane < start + BLOCK)
        a_ref[...] = jnp.where(within, 0.0, a_ref[...]) - change
        a_ref[pl.ds(start, BLOCK), :] = w
        return carry

    lax.fori_loop(0, ROWS // BLOCK, sweep, 0)
    result = -a_ref[...]
    packed = folded(result[0:HALF, 0:HALF], result[0:HALF, HALF:], result[HALF:, HALF:])
    for i in range(out_ref.shape[0]):
        out_ref[i] = packed


def unfold_kernel(packed_ref, out_ref):
    for i in range(out_ref.shape[0]):
        first, beside, last = unfolded(packed_ref[i])
        out_ref[i, 0:HALF, 0:HALF] = first
        out_ref[i, 0:HALF, HALF:] = beside
        out_ref[i, HALF:, 0:HALF] = beside.T[0 : ROWS - HALF, :]
        out_ref[i, HALF:, HALF:] = last[0 : ROWS - HALF, :]


def chain_kernel(date, dates, *refs):
    inv_ref, parts_ref, phi_ref, ex_ref, m_ref, index_ref, v_ref, disc_ref = refs[:8]
    refs = refs[8:]
    if date:
        next_ref = refs[0]
        refs = refs[1:]
    if date == dates - 1:
        coefs = jnp.zeros((ROWS, 128), f32)
    else:
        coefs = refs[0][...]
        refs = refs[1:]
    rhs = parts_ref[0]
    for i in range(1, parts_ref.shape[0]):
        rhs = rhs + parts_ref[i]
    if date == dates - 1:
        rhs = unfolded_row(rhs)
    product = inv_ref[date] * rhs
    coef = jnp.sum(product[:, 0:128] + product[:, 128:], axis=1, keepdims=True)
    coef = jnp.broadcast_to(coef, (ROWS, 128))
    out_ref, coef_ref, send_ref = refs
    continuation = []
    for c in range(0, v_ref.shape[1], 128):
        continuation.append(jnp.sum(coef * phi_ref[c // 128], axis=0, keepdims=True))
    continuation = jnp.concatenate(continuation, axis=1)
    exercise = ex_ref[date : date + 1, :]
    opened = jnp.where(index_ref[...] <= date, m_ref[date : date + 1, :].astype(f32), 0.0)
    weights = jax.nn.sigmoid((exercise - continuation) / temper_scale) * opened
    value = v_ref[...]
    value = value + weights * (exercise - value)
    if date:
        value = value * disc_ref[date - 1 : date, :]
        row = rhs_row(next_ref, value)
        for i in range(send_ref.shape[0]):
            send_ref[i] = row[0:1, :]
    else:
        total = jnp.broadcast_to(jnp.sum(value, axis=1, keepdims=True), (1, 128))
        for i in range(send_ref.shape[0]):
            send_ref[i] = total
    out_ref[...] = value
    coefs = jnp.where(lanes_of((ROWS, 128)) == date, coef, coefs)
    if date:
        coef_ref[...] = coefs
    else:
        for c in range(0, ROWS, 128):
            coef_ref[:, c : c + 128] = coefs[0:128, :].T if c == 0 else jnp.concatenate(
                [coefs[c:, :], jnp.zeros((128 - (ROWS - c), 128), f32)], axis=0
            ).T


def exchange(slots):
    return lax.all_to_all(slots, PATH, 0, 0, tiled=True)


def shards(states, itm_flags, terminal, strike, date_index):
    dates, factors, paths = states.shape
    size = lax.axis_size(PATH)
    sds = jax.ShapeDtypeStruct
    terminal = terminal.reshape(1, paths)
    date_index = date_index.reshape(1, paths)
    vmem = pltpu.VMEM
    limit = pltpu.CompilerParams(vmem_limit_bytes=24 << 20)
    stats = pl.pallas_call(
        stats_kernel,
        out_shape=vmem((size, factors, 128), f32),
        out_specs=WHOLE,
        compiler_params=limit,
        name="stats",
    )(states, itm_flags)
    stats = exchange(stats)
    exercise, discount = pl.pallas_call(
        swap_kernel,
        in_specs=[pl.BlockSpec(memory_space=pltpu.SMEM), WHOLE],
        out_specs=[WHOLE, WHOLE],
        out_shape=[vmem((dates, paths), f32), vmem((dates, paths), f32)],
        scratch_shapes=[pltpu.VMEM((factors, paths), f32)],
        compiler_params=limit,
        name="swap",
    )(strike, states)

    tiles = paths // 128
    slots, value = pl.pallas_call(
        gram_kernel,
        grid=(dates,),
        in_specs=[WHOLE] * 5,
        out_specs=[WHOLE] * 2,
        out_shape=[vmem((size, SLOT, 256), f32), vmem((1, paths), f32)],
        scratch_shapes=[
            pltpu.VMEM((CHUNK // 128, ROWS, 128), f32),
            pltpu.VMEM((CHUNK // 128, 32, 128), f32),
            pltpu.VMEM((256, 256), f32),
            pltpu.VMEM((1, 256), f32),
        ],
        compiler_params=limit,
        name="gram",
    )(near(stats), near(states), near(itm_flags), near(discount), near(terminal))
    phi = pl.pallas_call(
        basis_kernel,
        grid=(dates,),
        in_specs=[
            spec((size, factors, 128)),
            pl.BlockSpec((None, factors, paths), lambda i: (dates - 1 - i, 0, 0)),
            spec((dates, paths)),
        ],
        out_specs=[pl.BlockSpec(memory_space=pltpu.HBM)] * dates,
        out_shape=[pltpu.HBM((tiles, ROWS, 128), f32)] * dates,
        scratch_shapes=[
            pltpu.VMEM((2, tiles, ROWS, 128), f32),
            pltpu.VMEM((tiles, 32, 128), f32),
            pltpu.SemaphoreType.DMA((2,)),
        ],
        compiler_params=limit,
        name="basis",
    )(stats, states, itm_flags)
    slots = exchange(slots)
    inverse = pl.pallas_call(
        inverse_kernel,
        grid=(1,),
        in_specs=[WHOLE],
        out_specs=spec((size, SLOT, 256)),
        out_shape=pltpu.HBM((size, SLOT, 256), f32),
        scratch_shapes=[pltpu.VMEM((256, 256), f32)],
        compiler_params=limit,
        name="inverse",
    )(near(slots))
    inverse = exchange(inverse)
    inverse = pl.pallas_call(
        unfold_kernel,
        grid=(1,),
        in_specs=[spec((dates, SLOT, 256))],
        out_specs=WHOLE,
        out_shape=vmem((dates, ROWS, 256), f32),
        compiler_params=limit,
        name="unfold",
    )(inverse)
    received = slots[:, REST:SLOT, 0:HALF]
    coefs = None
    for date in range(dates - 1, -1, -1):
        args = [inverse, received, phi[date], exercise, itm_flags, date_index, value, discount]
        if date:
            args.append(phi[date - 1])
        if date < dates - 1:
            args.append(coefs)

        def kernel(*refs, date=date):
            chain_kernel(date, dates, *refs)

        value, coefs, send = pl.pallas_call(
            kernel,
            in_specs=[WHOLE] * len(args),
            out_specs=[WHOLE] * 3,
            out_shape=[
                vmem((1, paths), f32),
                vmem((ROWS, 128), f32),
                vmem((size, 1, 256), f32),
            ]
            if date
            else [sds((1, paths), f32), sds((128, 256), f32), sds((size, 1, 128), f32)],
            compiler_params=limit,
            name="chain",
        )(*(near(x) for x in args))
        received = exchange(send)
    book_price = jnp.sum(received[:, 0, 0:1], axis=0) / (paths * size)
    basis = 1 + factors + factors * (factors + 1) // 2
    coefficients = coefs[0:dates, 0:basis]
    return (value.reshape(paths), book_price, coefficients)


def solution(mesh):
    split = Mesh(mesh.devices.reshape(mesh.shape["book"], 4, 4), ("book", "path_0", "path_1"))
    return jax.shard_map(
        shards,
        mesh=split,
        in_specs=(
            P(None, None, BOOK_PATH),
            P(None, BOOK_PATH),
            P(BOOK_PATH),
            P("book"),
            P(BOOK_PATH),
        ),
        out_specs=(P(BOOK_PATH), P("book"), P("book", None)),
        check_vma=False,
    )
```

```python
import jax
import jax.numpy as jnp
from jax import lax
from jax.experimental import pallas as pl
from jax.experimental.pallas import tpu as pltpu
from jax.sharding import Mesh
from jax.sharding import PartitionSpec as P

PATH = ("path_0", "path_1")
BOOK_PATH = ("book", "path_0", "path_1")
ridge_weight = 0.05
temper_scale = 0.5
highest = lax.Precision.HIGHEST
f32 = jnp.float32
bf16 = jnp.bfloat16
NT = (((1,), (1,)), ((), ()))
TN = (((0,), (0,)), ((), ()))
ROWS = 240
HALF = 128
REST = 104
SLOT = 112
BLOCK = 16


def spec(shape, index=None):
    if index is None:
        index = (0,) * len(shape)
    return pl.BlockSpec(shape, lambda *_: index)


WHOLE = pl.BlockSpec(memory_space=pltpu.VMEM)


def near(x):
    return pltpu.with_memory_space_constraint(x, pltpu.VMEM)


def lanes_of(shape):
    return lax.broadcasted_iota(jnp.int32, shape, 1)


def rows_of(shape):
    return lax.broadcasted_iota(jnp.int32, shape, 0)


def stats_kernel(z_ref, m_ref, out_ref, sum_ref):
    step = pl.program_id(0)
    dates, factors, _ = z_ref.shape
    lane = lanes_of((factors, 128))

    @pl.when(step == 0)
    def _():
        sum_ref[...] = jnp.zeros_like(sum_ref)

    packed = sum_ref[0:factors, :]
    for i in range(dates):
        d = step * dates + i
        z = z_ref[i]
        m = m_ref[pl.ds(d, 1), :].astype(f32)
        mz = z * m
        packed = jnp.where(lane == 3 * d, jnp.sum(mz, axis=1, keepdims=True), packed)
        packed = jnp.where(lane == 3 * d + 1, jnp.sum(mz * z, axis=1, keepdims=True), packed)
        packed = jnp.where(lane == 3 * d + 2, jnp.sum(m, axis=1, keepdims=True), packed)
    sum_ref[0:factors, :] = packed
    groups = sum_ref[0:8] + pltpu.roll(sum_ref[8:16], 32, 1) + pltpu.roll(sum_ref[16:24], 64, 1)
    for i in range(out_ref.shape[0]):
        out_ref[i] = groups


def swap_kernel(strike_ref, z_ref, ex_ref, disc_ref, fac_ref):
    dates, factors, _ = z_ref.shape
    for d in range(dates):
        fac_ref[...] = 1.0 / (1.0 + 0.25 * (0.03 * jnp.exp(0.25 * z_ref[d])))
        first = fac_ref[0:1, :]
        disc = first
        total = first
        for j in range(1, factors):
            disc = disc * fac_ref[j : j + 1, :]
            total = total + disc
        disc_ref[d : d + 1, :] = first
        ex_ref[d : d + 1, :] = 100.0 * ((1.0 - disc) - strike_ref[0] * (0.25 * total))


def rhs_row(phi_ref, weights):
    acc = jnp.zeros((ROWS, 128), f32)
    for c in range(0, weights.shape[1], 128):
        acc = acc + phi_ref[c // 128] * weights[:, c : c + 128]
    row = lax.dot_general(
        jnp.ones((8, 128), f32), acc, NT, precision=highest, preferred_element_type=f32
    )
    return jnp.concatenate([row, jnp.zeros((8, 256 - ROWS), f32)], axis=1)


def column(stats, i):
    return jnp.sum(jnp.where(lanes_of(stats.shape) == i, stats, 0.0), axis=1, keepdims=True)


def moments(stats_ref, d, factors):
    stats = stats_ref[0]
    for i in range(1, stats_ref.shape[0]):
        stats = stats + stats_ref[i]
    stats = jnp.concatenate([stats, pltpu.roll(stats, 96, 1), pltpu.roll(stats, 64, 1)], axis=0)[0:factors]
    count = column(stats, 3 * d + 2)
    mean = column(stats, 3 * d) / count
    return mean, 1.0 / jnp.sqrt(column(stats, 3 * d + 1) / count - mean * mean + 1e-05)


def fill_basis(phi_ref, x_ref, z, m, mean, inverse):
    factors = z.shape[0]
    x_ref[0:factors, :] = (z - mean) * inverse * m
    phi_ref[0:1, :] = m
    phi_ref[1 : 1 + factors, :] = x_ref[0:factors, :]
    offset = 1 + factors
    for j in range(factors):
        left = jnp.broadcast_to(x_ref[j : j + 1, :], (8, 128))
        for k in range(0, factors - j, 8):
            phi_ref[offset + k : offset + k + 8, :] = left * x_ref[j + k : j + k + 8, :]
        offset += factors - j
    phi_ref[offset : offset + 8, :] = jnp.zeros((8, 128), f32)
    phi_ref[ROWS - 8 : ROWS, :] = jnp.zeros((8, 128), f32)


def basis_kernel(stats_ref, z_ref, m_ref, *refs):
    *phi_refs, phi_two_ref, x_ref, sems = refs
    step = pl.program_id(0)
    dates, paths = m_ref.shape
    d = dates - 1 - step
    side = step % 2

    def copy_of(half, date):
        return pltpu.make_async_copy(phi_two_ref.at[half], phi_refs[date], sems.at[half])

    @pl.when(step >= 2)
    def _():
        copy_of(side, 0).wait()

    mean, inverse = moments(stats_ref, d, z_ref.shape[0])
    m = m_ref[pl.ds(d, 1), :].astype(f32)
    for t in range(paths // 128):
        at = slice(t * 128, (t + 1) * 128)
        fill_basis(phi_two_ref.at[side, t], x_ref.at[t], z_ref[:, at], m[:, at], mean, inverse)
    for date in range(dates):

        @pl.when(d == date)
        def _(date=date):
            copy_of(side, date).start()

    @pl.when(step == dates - 1)
    def _():
        for half in range(2):
            copy_of(half, 0).wait()


def gram_kernel(stats_ref, z_all_ref, m_ref, disc_ref, term_ref, slots_ref, v_ref, *scratch):
    phi_ref, x_ref, gram_ref, rhs_ref, mean_ref, inverse_ref = scratch
    step = pl.program_id(0)
    dates, factors, paths = z_all_ref.shape
    d = dates - 1 - step

    @pl.when(step == 0)
    def _():
        x_ref[...] = jnp.zeros_like(x_ref)
        gram_ref[...] = jnp.zeros_like(gram_ref)
        v_ref[...] = term_ref[...] * disc_ref[dates - 1 : dates, :]
        for date in range(dates):
            mean, inverse = moments(stats_ref, date, factors)
            mean_ref[date] = jnp.broadcast_to(mean, (factors, 128))
            inverse_ref[date] = jnp.broadcast_to(inverse, (factors, 128))

    def fold(gram, date, first):
        row, lane = rows_of((HALF, HALF)), lanes_of((HALF, HALF))
        beside = jnp.where(lane < REST, gram[0:HALF, HALF:], 0.0)
        under = jnp.where((row < REST) & (lane < REST), gram[HALF:, HALF:], 0.0)
        rhs = jnp.sum(gram[ROWS : ROWS + 3, :], axis=0, keepdims=True)
        rhs = jnp.where(first, rhs, rhs_ref[...])
        rhs_ref[...] = rhs
        packed = folded(gram[0:HALF, 0:HALF], beside, under, rhs)
        slots_ref[date] = packed
        return packed

    packed = fold(gram_ref[...], d + 1, step == 1)
    flags = m_ref[pl.ds(d, 1), :].astype(f32)
    values = jnp.where(step == 0, v_ref[...], 0.0)
    mean, inverse = mean_ref[d], inverse_ref[d]
    total = None
    for pair in range(0, paths // 128, 2):
        hi, lo = [], []
        for t in (pair, pair + 1):
            at = slice(t * 128, (t + 1) * 128)
            fill_basis(phi_ref.at[t], x_ref.at[t], z_all_ref[d, :, at], flags[:, at], mean, inverse)
            phi = phi_ref[t]
            high = phi.astype(bf16)
            low = (phi - high.astype(f32)).astype(bf16)
            value = values[:, at]
            one = value.astype(bf16).astype(f32)
            two = (value - one).astype(bf16).astype(f32)
            three = value - one - two
            row = rows_of((256 - ROWS, 128))
            under = jnp.where(row == 0, one, jnp.where(row == 1, two, jnp.where(row == 2, three, 0.0)))
            hi.append(jnp.concatenate([high, under.astype(bf16)], axis=0))
            lo.append(jnp.concatenate([low, jnp.zeros((256 - ROWS, 128), bf16)], axis=0))
        hi = jnp.concatenate(hi, axis=1)
        lo = jnp.concatenate(lo, axis=1)
        both = lax.dot_general(
            jnp.concatenate([hi, lo], axis=0), hi, NT, preferred_element_type=f32
        )
        part = both[0:256] + both[256:] + lax.dot_general(hi, lo, NT, preferred_element_type=f32)
        total = part if total is None else total + part
    gram_ref[...] = total

    @pl.when(step == 1)
    def _():
        for i in range(dates, slots_ref.shape[0]):
            slots_ref[i] = packed

    @pl.when(step == dates - 1)
    def _():
        fold(gram_ref[...], 0, False)


def folded(first, beside, last, rhs=None):
    row, lane = rows_of((HALF, HALF)), lanes_of((HALF, HALF))
    left = jnp.where(row <= lane, first, last)
    low_lane = lanes_of((8, HALF))
    low = left[REST:SLOT]
    low = jnp.where(low_lane < 16, pltpu.roll(first[SLOT : SLOT + 8], 16, 1), low)
    low = jnp.where((low_lane >= 16) & (low_lane < 32), pltpu.roll(first[SLOT + 8 :], 32, 1), low)
    if rhs is not None:
        low_row = rows_of((8, HALF))
        for i in range(4):
            piece = pltpu.roll(jnp.broadcast_to(rhs, (8, 256)), (32 - 72 * i) % 256, 1)[:, 0:HALF]
            low = jnp.where((low_row == i) & (low_lane >= 32) & (low_lane < REST), piece, low)
    left = jnp.concatenate([left[0:REST], low], axis=0)
    diagonal = jnp.sum(jnp.where(row == lane, last, 0.0), axis=1, keepdims=True)
    right = jnp.where(lane < REST, beside, pltpu.roll(beside.T, HALF - 8, 1))
    right = jnp.where(lane == 120, diagonal, right)[0:SLOT]
    return jnp.concatenate([left, right], axis=1)


def unfolded(packed):
    row, lane = rows_of((HALF, HALF)), lanes_of((HALF, HALF))
    none = jnp.zeros((HALF - SLOT, HALF), f32)
    left = jnp.concatenate([packed[:, 0:HALF], none], axis=0)
    right = jnp.concatenate([packed[:, HALF:], none], axis=0)
    low = left[REST:SLOT]
    corner = jnp.concatenate(
        [left[0:SLOT], pltpu.roll(low, HALF - 16, 1), pltpu.roll(low, HALF - 32, 1)], axis=0
    )
    turned = left.T
    first = jnp.where(row <= lane, left, turned)
    first = jnp.where((row >= SLOT) & (lane >= SLOT), corner, first)
    diagonal = jnp.sum(jnp.where(lane == 120, right, 0.0), axis=1, keepdims=True)
    last = jnp.where(row > lane, left, turned)
    last = jnp.where(row == lane, diagonal, last)
    last = jnp.where((row < REST) & (lane < REST), last, 0.0)
    beside = jnp.where(row < SLOT, right, pltpu.roll(right, 8, 1).T)
    beside = jnp.where(lane < REST, beside, 0.0)
    return first, beside, last


def unfolded_row(low):
    lane = lanes_of((1, 256))
    wide = jnp.concatenate([low, jnp.zeros((8, HALF), f32)], axis=1)
    total = jnp.zeros((1, 256), f32)
    for i in range(4):
        piece = pltpu.roll(wide, (72 * i - 32) % 256, 1)[i : i + 1]
        total = jnp.where((lane >= 72 * i) & (lane < min(72 * i + 72, 231)), piece, total)
    return total


def inverse_kernel(parts_ref, out_ref, rhs_ref, a_ref):
    basis = 231
    packed = parts_ref[0]
    for i in range(1, parts_ref.shape[0]):
        packed = packed + parts_ref[i]
    rhs_ref[0] = unfolded_row(packed[REST:SLOT, 0:HALF])
    first, beside, last = unfolded(packed)
    a_ref[0:HALF, 0:HALF] = first
    a_ref[0:HALF, HALF:] = beside
    a_ref[HALF:, 0:HALF] = beside.T
    a_ref[HALF:, HALF:] = last
    count = packed[0:1, 0:1]
    row, lane = rows_of((256, 256)), lanes_of((256, 256))
    added = jnp.where(row < basis, ridge_weight * count, 1.0)
    a_ref[...] = a_ref[...] + jnp.where(row == lane, added, 0.0)
    lane_a = lanes_of((BLOCK, 128))
    lane_b = lane_a + 128
    row_a = rows_of((BLOCK, 128))
    lane_r = lanes_of((BLOCK, 256))

    def split(x):
        one = x.astype(bf16)
        rest = x - one.astype(f32)
        two = rest.astype(bf16)
        return one, two, (rest - two.astype(f32)).astype(bf16)

    def sweep(i, carry):
        start = pl.multiple_of(i * BLOCK, BLOCK)
        panel = a_ref[pl.ds(start, BLOCK), :]
        ra, rb = panel[:, 0:128], panel[:, 128:]
        cols = []
        for c in range(BLOCK):
            both = jnp.where(lane_a == start + c, ra, 0.0) + jnp.where(lane_b == start + c, rb, 0.0)
            cols.append(jnp.broadcast_to(jnp.sum(both, axis=1, keepdims=True), (BLOCK, 128)))
        for k in range(BLOCK):
            pivot = 1.0 / cols[k][k : k + 1, :]
            here = row_a == k
            unit = jnp.where(here, 1.0, 0.0)
            ra = jnp.where(lane_a == start + k, unit, ra)
            rb = jnp.where(lane_b == start + k, unit, rb)
            row_k = ra[k : k + 1, :] * pivot
            ra = jnp.where(here, row_k, ra - cols[k] * row_k)
            row_k = rb[k : k + 1, :] * pivot
            rb = jnp.where(here, row_k, rb - cols[k] * row_k)
            for c in range(k + 1, BLOCK):
                f = cols[c][k : k + 1, :] * pivot
                cols[c] = jnp.where(here, f, cols[c] - cols[k] * f)
        inside = (lane_r >= start) & (lane_r < start + BLOCK)
        w = jnp.concatenate([ra, rb], axis=1)
        w = jnp.where(inside, -w, w)
        r1, r2, r3 = split(panel)
        w1, w2, w3 = split(w)
        left = jnp.concatenate([r1, r1, r2, r2, r1, r3], axis=0)
        right = jnp.concatenate([w1, w2, w1, w2, w3, w1], axis=0)
        change = lax.dot_general(left, right, TN, preferred_element_type=f32)
        within = (lane >= start) & (lane < start + BLOCK)
        a_ref[...] = jnp.where(within, 0.0, a_ref[...]) - change
        a_ref[pl.ds(start, BLOCK), :] = w
        return carry

    lax.fori_loop(0, ROWS // BLOCK, sweep, 0)
    result = -a_ref[...]
    packed = folded(result[0:HALF, 0:HALF], result[0:HALF, HALF:], result[HALF:, HALF:])
    for i in range(out_ref.shape[0]):
        out_ref[i] = packed


def unfold_kernel(packed_ref, out_ref):
    for i in range(out_ref.shape[0]):
        first, beside, last = unfolded(packed_ref[i])
        out_ref[i, 0:HALF, 0:HALF] = first
        out_ref[i, 0:HALF, HALF:] = beside
        out_ref[i, HALF:, 0:HALF] = beside.T[0 : ROWS - HALF, :]
        out_ref[i, HALF:, HALF:] = last[0 : ROWS - HALF, :]


def chain_kernel(date, dates, *refs):
    inv_ref, parts_ref, phi_ref, ex_ref, m_ref, index_ref, v_ref, disc_ref = refs[:8]
    refs = refs[8:]
    if date:
        next_ref = refs[0]
        refs = refs[1:]
    if date == dates - 1:
        coefs = jnp.zeros((ROWS, 128), f32)
    else:
        coefs = refs[0][...]
        refs = refs[1:]
    rhs = parts_ref[0]
    for i in range(1, parts_ref.shape[0]):
        rhs = rhs + parts_ref[i]
    product = inv_ref[date] * rhs
    coef = jnp.sum(product[:, 0:128] + product[:, 128:], axis=1, keepdims=True)
    coef = jnp.broadcast_to(coef, (ROWS, 128))
    out_ref, coef_ref, send_ref = refs
    continuation = []
    for c in range(0, v_ref.shape[1], 128):
        continuation.append(jnp.sum(coef * phi_ref[c // 128], axis=0, keepdims=True))
    continuation = jnp.concatenate(continuation, axis=1)
    exercise = ex_ref[date : date + 1, :]
    opened = jnp.where(index_ref[...] <= date, m_ref[date : date + 1, :].astype(f32), 0.0)
    weights = jax.nn.sigmoid((exercise - continuation) / temper_scale) * opened
    value = v_ref[...]
    value = value + weights * (exercise - value)
    if date:
        value = value * disc_ref[date - 1 : date, :]
        row = rhs_row(next_ref, value)
        for i in range(send_ref.shape[0]):
            send_ref[i] = row[0:1, :]
    else:
        total = jnp.broadcast_to(jnp.sum(value, axis=1, keepdims=True), (1, 128))
        for i in range(send_ref.shape[0]):
            send_ref[i] = total
    out_ref[...] = value
    coefs = jnp.where(lanes_of((ROWS, 128)) == date, coef, coefs)
    if date:
        coef_ref[...] = coefs
    else:
        for c in range(0, ROWS, 128):
            coef_ref[:, c : c + 128] = coefs[0:128, :].T if c == 0 else jnp.concatenate(
                [coefs[c:, :], jnp.zeros((128 - (ROWS - c), 128), f32)], axis=0
            ).T


def exchange(slots):
    return lax.all_to_all(slots, PATH, 0, 0, tiled=True)


def shards(states, itm_flags, terminal, strike, date_index):
    dates, factors, paths = states.shape
    size = lax.axis_size(PATH)
    sds = jax.ShapeDtypeStruct
    terminal = terminal.reshape(1, paths)
    date_index = date_index.reshape(1, paths)
    vmem = pltpu.VMEM
    limit = pltpu.CompilerParams(vmem_limit_bytes=24 << 20)
    stats = pl.pallas_call(
        stats_kernel,
        grid=(2,),
        in_specs=[
            pl.BlockSpec((dates // 2, factors, paths), lambda i: (i, 0, 0)),
            spec((dates, paths)),
        ],
        out_shape=vmem((size, 8, 128), f32),
        out_specs=WHOLE,
        scratch_shapes=[pltpu.VMEM((24, 128), f32)],
        compiler_params=limit,
        name="stats",
    )(pltpu.with_memory_space_constraint(states, pltpu.HBM), pltpu.with_memory_space_constraint(itm_flags, pltpu.HBM))
    stats = exchange(stats)
    exercise, discount = pl.pallas_call(
        swap_kernel,
        in_specs=[pl.BlockSpec(memory_space=pltpu.SMEM), WHOLE],
        out_specs=[WHOLE, WHOLE],
        out_shape=[vmem((dates, paths), f32), vmem((dates, paths), f32)],
        scratch_shapes=[pltpu.VMEM((factors, paths), f32)],
        compiler_params=limit,
        name="swap",
    )(strike, states)

    tiles = paths // 128
    slots, value = pl.pallas_call(
        gram_kernel,
        grid=(dates,),
        in_specs=[WHOLE] * 5,
        out_specs=[WHOLE] * 2,
        out_shape=[vmem((size, SLOT, 256), f32), vmem((1, paths), f32)],
        scratch_shapes=[
            pltpu.VMEM((tiles, ROWS, 128), f32),
            pltpu.VMEM((tiles, 32, 128), f32),
            pltpu.VMEM((256, 256), f32),
            pltpu.VMEM((1, 256), f32),
            pltpu.VMEM((dates, factors, 128), f32),
            pltpu.VMEM((dates, factors, 128), f32),
        ],
        compiler_params=limit,
        name="gram",
    )(near(stats), near(states), near(itm_flags), near(discount), near(terminal))
    phi = pl.pallas_call(
        basis_kernel,
        grid=(dates,),
        in_specs=[
            spec((size, 8, 128)),
            pl.BlockSpec((None, factors, paths), lambda i: (dates - 1 - i, 0, 0)),
            spec((dates, paths)),
        ],
        out_specs=[pl.BlockSpec(memory_space=pltpu.HBM)] * dates,
        out_shape=[pltpu.HBM((tiles, ROWS, 128), f32)] * dates,
        scratch_shapes=[
            pltpu.VMEM((2, tiles, ROWS, 128), f32),
            pltpu.VMEM((tiles, 32, 128), f32),
            pltpu.SemaphoreType.DMA((2,)),
        ],
        compiler_params=limit,
        name="basis",
    )(stats, states, itm_flags)
    slots = exchange(slots)
    inverse, received = pl.pallas_call(
        inverse_kernel,
        grid=(1,),
        in_specs=[WHOLE],
        out_specs=[spec((size, SLOT, 256)), WHOLE],
        out_shape=[pltpu.HBM((size, SLOT, 256), f32), vmem((1, 1, 256), f32)],
        scratch_shapes=[pltpu.VMEM((256, 256), f32)],
        compiler_params=limit,
        name="inverse",
    )(near(slots))
    inverse = exchange(inverse)
    inverse = pl.pallas_call(
        unfold_kernel,
        grid=(1,),
        in_specs=[spec((dates, SLOT, 256))],
        out_specs=WHOLE,
        out_shape=vmem((dates, ROWS, 256), f32),
        compiler_params=limit,
        name="unfold",
    )(inverse)
    coefs = None
    for date in range(dates - 1, -1, -1):
        args = [inverse, received, phi[date], exercise, itm_flags, date_index, value, discount]
        if date:
            args.append(phi[date - 1])
        if date < dates - 1:
            args.append(coefs)

        def kernel(*refs, date=date):
            chain_kernel(date, dates, *refs)

        value, coefs, send = pl.pallas_call(
            kernel,
            in_specs=[WHOLE] * len(args),
            out_specs=[WHOLE] * 3,
            out_shape=[
                vmem((1, paths), f32),
                vmem((ROWS, 128), f32),
                vmem((size, 1, 256), f32),
            ]
            if date
            else [sds((1, paths), f32), sds((128, 256), f32), sds((size, 1, 128), f32)],
            compiler_params=limit,
            name="chain",
        )(*(near(x) for x in args))
        received = exchange(send)
    book_price = jnp.sum(received[:, 0, 0:1], axis=0) / (paths * size)
    basis = 1 + factors + factors * (factors + 1) // 2
    coefficients = coefs[0:dates, 0:basis]
    return (value.reshape(paths), book_price, coefficients)


def solution(mesh):
    split = Mesh(mesh.devices.reshape(mesh.shape["book"], 4, 4), ("book", "path_0", "path_1"))
    return jax.shard_map(
        shards,
        mesh=split,
        in_specs=(
            P(None, None, BOOK_PATH),
            P(None, BOOK_PATH),
            P(BOOK_PATH),
            P("book"),
            P(BOOK_PATH),
        ),
        out_specs=(P(BOOK_PATH), P("book"), P("book", None)),
        check_vma=False,
    )
```

```python
import jax
import jax.numpy as jnp
from jax import lax
from jax.experimental import pallas as pl
from jax.experimental.pallas import tpu as pltpu
from jax.sharding import Mesh
from jax.sharding import PartitionSpec as P

PATH = ("path_0", "path_1")
BOOK_PATH = ("book", "path_0", "path_1")
ridge_weight = 0.05
temper_scale = 0.5
highest = lax.Precision.HIGHEST
f32 = jnp.float32
bf16 = jnp.bfloat16
NT = (((1,), (1,)), ((), ()))
TN = (((0,), (0,)), ((), ()))
ROWS = 240
HALF = 128
REST = 104
SLOT = 112
SENT = 64
PIECES = 6
WIDE = 256 * 9
BLOCK = 16


def spec(shape, index=None):
    if index is None:
        index = (0,) * len(shape)
    return pl.BlockSpec(shape, lambda *_: index)


WHOLE = pl.BlockSpec(memory_space=pltpu.VMEM)


def near(x):
    return pltpu.with_memory_space_constraint(x, pltpu.VMEM)


def lanes_of(shape):
    return lax.broadcasted_iota(jnp.int32, shape, 1)


def rows_of(shape):
    return lax.broadcasted_iota(jnp.int32, shape, 0)


def stats_kernel(z_ref, m_ref, out_ref, sum_ref):
    step = pl.program_id(0)
    dates, factors, _ = z_ref.shape
    lane = lanes_of((factors, 128))

    @pl.when(step == 0)
    def _():
        sum_ref[...] = jnp.zeros_like(sum_ref)

    packed = sum_ref[0:factors, :]
    for i in range(dates):
        d = step * dates + i
        z = z_ref[i]
        m = m_ref[pl.ds(d, 1), :].astype(f32)
        mz = z * m
        packed = jnp.where(lane == 3 * d, jnp.sum(mz, axis=1, keepdims=True), packed)
        packed = jnp.where(lane == 3 * d + 1, jnp.sum(mz * z, axis=1, keepdims=True), packed)
        packed = jnp.where(lane == 3 * d + 2, jnp.sum(m, axis=1, keepdims=True), packed)
    sum_ref[0:factors, :] = packed
    groups = sum_ref[0:8] + pltpu.roll(sum_ref[8:16], 32, 1) + pltpu.roll(sum_ref[16:24], 64, 1)
    for i in range(out_ref.shape[0]):
        out_ref[i] = groups


def swap_kernel(strike_ref, z_ref, ex_ref, disc_ref, fac_ref):
    dates, factors, _ = z_ref.shape
    for d in range(dates):
        fac_ref[...] = 1.0 / (1.0 + 0.25 * (0.03 * jnp.exp(0.25 * z_ref[d])))
        first = fac_ref[0:1, :]
        disc = first
        total = first
        for j in range(1, factors):
            disc = disc * fac_ref[j : j + 1, :]
            total = total + disc
        disc_ref[d : d + 1, :] = first
        ex_ref[d : d + 1, :] = 100.0 * ((1.0 - disc) - strike_ref[0] * (0.25 * total))


def rhs_row(phi_ref, weights):
    acc = jnp.zeros((ROWS, 128), f32)
    for c in range(0, weights.shape[1], 128):
        acc = acc + phi_ref[c // 128] * weights[:, c : c + 128]
    row = lax.dot_general(
        jnp.ones((8, 128), f32), acc, NT, precision=highest, preferred_element_type=f32
    )
    return jnp.concatenate([row, jnp.zeros((8, 256 - ROWS), f32)], axis=1)


def column(stats, i):
    return jnp.sum(jnp.where(lanes_of(stats.shape) == i, stats, 0.0), axis=1, keepdims=True)


def moments(stats_ref, d, factors):
    stats = stats_ref[0]
    for i in range(1, stats_ref.shape[0]):
        stats = stats + stats_ref[i]
    stats = jnp.concatenate([stats, pltpu.roll(stats, 96, 1), pltpu.roll(stats, 64, 1)], axis=0)[0:factors]
    count = column(stats, 3 * d + 2)
    mean = column(stats, 3 * d) / count
    return mean, 1.0 / jnp.sqrt(column(stats, 3 * d + 1) / count - mean * mean + 1e-05)


def fill_basis(phi_ref, x_ref, z, m, mean, inverse):
    factors = z.shape[0]
    x_ref[0:factors, :] = (z - mean) * inverse * m
    phi_ref[0:1, :] = m
    phi_ref[1 : 1 + factors, :] = x_ref[0:factors, :]
    offset = 1 + factors
    for j in range(factors):
        left = jnp.broadcast_to(x_ref[j : j + 1, :], (8, 128))
        for k in range(0, factors - j, 8):
            phi_ref[offset + k : offset + k + 8, :] = left * x_ref[j + k : j + k + 8, :]
        offset += factors - j
    phi_ref[offset : offset + 8, :] = jnp.zeros((8, 128), f32)
    phi_ref[ROWS - 8 : ROWS, :] = jnp.zeros((8, 128), f32)


def basis_kernel(stats_ref, z_ref, m_ref, *refs):
    *phi_refs, phi_two_ref, x_ref, sems = refs
    step = pl.program_id(0)
    dates, paths = m_ref.shape
    d = dates - 1 - step
    side = step % 2

    def copy_of(half, date):
        return pltpu.make_async_copy(phi_two_ref.at[half], phi_refs[date], sems.at[half])

    @pl.when(step >= 2)
    def _():
        copy_of(side, 0).wait()

    mean, inverse = moments(stats_ref, d, z_ref.shape[0])
    m = m_ref[pl.ds(d, 1), :].astype(f32)
    for t in range(paths // 128):
        at = slice(t * 128, (t + 1) * 128)
        fill_basis(phi_two_ref.at[side, t], x_ref.at[t], z_ref[:, at], m[:, at], mean, inverse)
    for date in range(dates):

        @pl.when(d == date)
        def _(date=date):
            copy_of(side, date).start()

    @pl.when(step == dates - 1)
    def _():
        for half in range(2):
            copy_of(half, 0).wait()


def gram_kernel(stats_ref, z_all_ref, m_ref, disc_ref, term_ref, slots_ref, v_ref, *scratch):
    phi_ref, x_ref, gram_ref, rhs_ref, mean_ref, inverse_ref = scratch
    step = pl.program_id(0)
    dates, factors, paths = z_all_ref.shape
    d = dates - 1 - step

    @pl.when(step == 0)
    def _():
        x_ref[...] = jnp.zeros_like(x_ref)
        gram_ref[...] = jnp.zeros_like(gram_ref)
        v_ref[...] = term_ref[...] * disc_ref[dates - 1 : dates, :]
        for date in range(dates):
            mean, inverse = moments(stats_ref, date, factors)
            mean_ref[date] = jnp.broadcast_to(mean, (factors, 128))
            inverse_ref[date] = jnp.broadcast_to(inverse, (factors, 128))

    def fold(gram, date, first):
        row, lane = rows_of((HALF, HALF)), lanes_of((HALF, HALF))
        beside = jnp.where(lane < REST, gram[0:HALF, HALF:], 0.0)
        under = jnp.where((row < REST) & (lane < REST), gram[HALF:, HALF:], 0.0)
        rhs = jnp.sum(gram[ROWS : ROWS + 3, :], axis=0, keepdims=True)
        rhs = jnp.where(first, rhs, rhs_ref[...])
        rhs_ref[...] = rhs
        packed = folded(gram[0:HALF, 0:HALF], beside, under, rhs)
        slots_ref[date] = packed
        again = 2 * dates - 1 - date
        slots_ref[jnp.where(again < slots_ref.shape[0], again, date)] = packed

    fold(gram_ref[...], d + 1, step == 1)
    flags = m_ref[pl.ds(d, 1), :].astype(f32)
    values = jnp.where(step == 0, v_ref[...], 0.0)
    mean, inverse = mean_ref[d], inverse_ref[d]
    total = None
    for pair in range(0, paths // 128, 2):
        hi, lo = [], []
        for t in (pair, pair + 1):
            at = slice(t * 128, (t + 1) * 128)
            fill_basis(phi_ref.at[t], x_ref.at[t], z_all_ref[d, :, at], flags[:, at], mean, inverse)
            phi = phi_ref[t]
            high = phi.astype(bf16)
            low = (phi - high.astype(f32)).astype(bf16)
            value = values[:, at]
            one = value.astype(bf16).astype(f32)
            two = (value - one).astype(bf16).astype(f32)
            three = value - one - two
            row = rows_of((256 - ROWS, 128))
            under = jnp.where(row == 0, one, jnp.where(row == 1, two, jnp.where(row == 2, three, 0.0)))
            hi.append(jnp.concatenate([high, under.astype(bf16)], axis=0))
            lo.append(jnp.concatenate([low, jnp.zeros((256 - ROWS, 128), bf16)], axis=0))
        hi = jnp.concatenate(hi, axis=1)
        lo = jnp.concatenate(lo, axis=1)
        both = lax.dot_general(
            jnp.concatenate([hi, lo], axis=0), hi, NT, preferred_element_type=f32
        )
        part = both[0:256] + both[256:] + lax.dot_general(hi, lo, NT, preferred_element_type=f32)
        total = part if total is None else total + part
    gram_ref[...] = total

    @pl.when(step == dates - 1)
    def _():
        fold(gram_ref[...], 0, False)


def folded(first, beside, last, rhs=None):
    row, lane = rows_of((HALF, HALF)), lanes_of((HALF, HALF))
    left = jnp.where(row <= lane, first, last)
    low_lane = lanes_of((8, HALF))
    low = left[REST:SLOT]
    low = jnp.where(low_lane < 16, pltpu.roll(first[SLOT : SLOT + 8], 16, 1), low)
    low = jnp.where((low_lane >= 16) & (low_lane < 32), pltpu.roll(first[SLOT + 8 :], 32, 1), low)
    if rhs is not None:
        low_row = rows_of((8, HALF))
        for i in range(4):
            piece = pltpu.roll(jnp.broadcast_to(rhs, (8, 256)), (32 - 72 * i) % 256, 1)[:, 0:HALF]
            low = jnp.where((low_row == i) & (low_lane >= 32) & (low_lane < REST), piece, low)
    left = jnp.concatenate([left[0:REST], low], axis=0)
    diagonal = jnp.sum(jnp.where(row == lane, last, 0.0), axis=1, keepdims=True)
    right = jnp.where(lane < REST, beside, pltpu.roll(beside.T, HALF - 8, 1))
    right = jnp.where(lane == 120, diagonal, right)[0:SLOT]
    return jnp.concatenate([left, right], axis=1)


def unfolded(packed):
    row, lane = rows_of((HALF, HALF)), lanes_of((HALF, HALF))
    none = jnp.zeros((HALF - SLOT, HALF), f32)
    left = jnp.concatenate([packed[:, 0:HALF], none], axis=0)
    right = jnp.concatenate([packed[:, HALF:], none], axis=0)
    low = left[REST:SLOT]
    corner = jnp.concatenate(
        [left[0:SLOT], pltpu.roll(low, HALF - 16, 1), pltpu.roll(low, HALF - 32, 1)], axis=0
    )
    turned = left.T
    first = jnp.where(row <= lane, left, turned)
    first = jnp.where((row >= SLOT) & (lane >= SLOT), corner, first)
    diagonal = jnp.sum(jnp.where(lane == 120, right, 0.0), axis=1, keepdims=True)
    last = jnp.where(row > lane, left, turned)
    last = jnp.where(row == lane, diagonal, last)
    last = jnp.where((row < REST) & (lane < REST), last, 0.0)
    beside = jnp.where(row < SLOT, right, pltpu.roll(right, 8, 1).T)
    beside = jnp.where(lane < REST, beside, 0.0)
    return first, beside, last


def unfolded_row(low):
    lane = lanes_of((1, 256))
    wide = jnp.concatenate([low, jnp.zeros((8, HALF), f32)], axis=1)
    total = jnp.zeros((1, 256), f32)
    for i in range(4):
        piece = pltpu.roll(wide, (72 * i - 32) % 256, 1)[i : i + 1]
        total = jnp.where((lane >= 72 * i) & (lane < min(72 * i + 72, 231)), piece, total)
    return total


def inverse_kernel(dates, place_ref, parts_ref, out_ref, rest_ref, rhs_ref, a_ref):
    basis = 231
    packed = parts_ref[0]
    for i in range(1, parts_ref.shape[0]):
        packed = packed + parts_ref[i]
    rhs_ref[0] = unfolded_row(packed[REST:SLOT, 0:HALF])
    first, beside, last = unfolded(packed)
    a_ref[0:HALF, 0:HALF] = first
    a_ref[0:HALF, HALF:] = beside
    a_ref[HALF:, 0:HALF] = beside.T
    a_ref[HALF:, HALF:] = last
    count = packed[0:1, 0:1]
    row, lane = rows_of((256, 256)), lanes_of((256, 256))
    added = jnp.where(row < basis, ridge_weight * count, 1.0)
    a_ref[...] = a_ref[...] + jnp.where(row == lane, added, 0.0)
    lane_a = lanes_of((BLOCK, 128))
    lane_b = lane_a + 128
    row_a = rows_of((BLOCK, 128))
    lane_r = lanes_of((BLOCK, 256))

    def split(x):
        one = x.astype(bf16)
        rest = x - one.astype(f32)
        two = rest.astype(bf16)
        return one, two, (rest - two.astype(f32)).astype(bf16)

    def sweep(i, carry):
        start = pl.multiple_of(i * BLOCK, BLOCK)
        panel = a_ref[pl.ds(start, BLOCK), :]
        ra, rb = panel[:, 0:128], panel[:, 128:]
        cols = []
        for c in range(BLOCK):
            both = jnp.where(lane_a == start + c, ra, 0.0) + jnp.where(lane_b == start + c, rb, 0.0)
            cols.append(jnp.broadcast_to(jnp.sum(both, axis=1, keepdims=True), (BLOCK, 128)))
        for k in range(BLOCK):
            pivot = 1.0 / cols[k][k : k + 1, :]
            here = row_a == k
            unit = jnp.where(here, 1.0, 0.0)
            ra = jnp.where(lane_a == start + k, unit, ra)
            rb = jnp.where(lane_b == start + k, unit, rb)
            row_k = ra[k : k + 1, :] * pivot
            ra = jnp.where(here, row_k, ra - cols[k] * row_k)
            row_k = rb[k : k + 1, :] * pivot
            rb = jnp.where(here, row_k, rb - cols[k] * row_k)
            for c in range(k + 1, BLOCK):
                f = cols[c][k : k + 1, :] * pivot
                cols[c] = jnp.where(here, f, cols[c] - cols[k] * f)
        inside = (lane_r >= start) & (lane_r < start + BLOCK)
        w = jnp.concatenate([ra, rb], axis=1)
        w = jnp.where(inside, -w, w)
        r1, r2, r3 = split(panel)
        w1, w2, w3 = split(w)
        left = jnp.concatenate([r1, r1, r2, r2, r1, r3], axis=0)
        right = jnp.concatenate([w1, w2, w1, w2, w3, w1], axis=0)
        change = lax.dot_general(left, right, TN, preferred_element_type=f32)
        within = (lane >= start) & (lane < start + BLOCK)
        a_ref[...] = jnp.where(within, 0.0, a_ref[...]) - change
        a_ref[pl.ds(start, BLOCK), :] = w
        return carry

    lax.fori_loop(0, ROWS // BLOCK, sweep, 0)
    result = -a_ref[...]
    packed = folded(result[0:HALF, 0:HALF], result[0:HALF, HALF:], result[HALF:, HALF:])
    own = jnp.broadcast_to(place_ref[...] < dates, (SENT, 256))
    sent = jnp.where(own, packed[0:SENT], packed[SLOT - SENT :])
    for i in range(out_ref.shape[0]):
        out_ref[i] = sent
    rest_ref[...] = packed[SENT:SLOT]


def pieces_kernel(rest_ref, *out_refs):
    for p, out_ref in enumerate(out_refs):
        for i in range(out_ref.shape[0]):
            out_ref[i, :, 0:256] = jnp.zeros((1, 256), f32)
            for r in range(8):
                row = 8 * p + r
                out_ref[i, :, 256 * (1 + r) : 256 * (2 + r)] = rest_ref[row : row + 1, :]


def unfold_pairs_kernel(first_date, dates, parts_ref, out_ref):
    for i in range(out_ref.shape[0]):
        date = first_date + i
        rest = parts_ref[2 * dates - 1 - date]
        write_unfolded(jnp.concatenate([parts_ref[date], rest[2 * SENT - SLOT :]], axis=0), out_ref.at[i])


def unfold_pieces_kernel(parts_ref, *refs):
    *piece_refs, out_ref, packed_ref = refs
    for i in range(out_ref.shape[0]):
        packed_ref[i, 0:SENT, :] = parts_ref[i]
        for p, piece_ref in enumerate(piece_refs):
            for r in range(8):
                row = SENT + 8 * p + r
                packed_ref[i, row : row + 1, :] = piece_ref[i, :, 256 * (1 + r) : 256 * (2 + r)]
        write_unfolded(packed_ref[i], out_ref.at[i])


def write_unfolded(packed, out_ref):
    first, beside, last = unfolded(packed)
    out_ref[0:HALF, 0:HALF] = first
    out_ref[0:HALF, HALF:] = beside
    out_ref[HALF:, 0:HALF] = beside.T[0 : ROWS - HALF, :]
    out_ref[HALF:, HALF:] = last[0 : ROWS - HALF, :]


def chain_kernel(date, dates, first_date, *refs):
    inv_ref, parts_ref, phi_ref, ex_ref, m_ref, index_ref, v_ref, disc_ref = refs[:8]
    refs = refs[8:]
    if date:
        next_ref = refs[0]
        refs = refs[1:]
    if date == dates - 1:
        coefs = jnp.zeros((ROWS, 128), f32)
    else:
        coefs = refs[0][...]
        refs = refs[1:]
    if len(refs) == 4:
        refs = refs[1:]
    rhs = parts_ref[0, :, 0:256]
    for i in range(1, parts_ref.shape[0]):
        rhs = rhs + parts_ref[i, :, 0:256]
    product = inv_ref[date - first_date] * rhs
    coef = jnp.sum(product[:, 0:128] + product[:, 128:], axis=1, keepdims=True)
    coef = jnp.broadcast_to(coef, (ROWS, 128))
    out_ref, coef_ref, send_ref = refs
    continuation = []
    for c in range(0, v_ref.shape[1], 128):
        continuation.append(jnp.sum(coef * phi_ref[c // 128], axis=0, keepdims=True))
    continuation = jnp.concatenate(continuation, axis=1)
    exercise = ex_ref[date : date + 1, :]
    opened = jnp.where(index_ref[...] <= date, m_ref[date : date + 1, :].astype(f32), 0.0)
    weights = jax.nn.sigmoid((exercise - continuation) / temper_scale) * opened
    value = v_ref[...]
    value = value + weights * (exercise - value)
    if date:
        value = value * disc_ref[date - 1 : date, :]
        row = rhs_row(next_ref, value)
        for i in range(send_ref.shape[0]):
            send_ref[i, :, 0:256] = row[0:1, :]
    else:
        total = jnp.broadcast_to(jnp.sum(value, axis=1, keepdims=True), (1, 128))
        for i in range(send_ref.shape[0]):
            send_ref[i] = total
    out_ref[...] = value
    coefs = jnp.where(lanes_of((ROWS, 128)) == date, coef, coefs)
    if date:
        coef_ref[...] = coefs
    else:
        for c in range(0, ROWS, 128):
            coef_ref[:, c : c + 128] = coefs[0:128, :].T if c == 0 else jnp.concatenate(
                [coefs[c:, :], jnp.zeros((128 - (ROWS - c), 128), f32)], axis=0
            ).T


def exchange(slots):
    return lax.all_to_all(slots, PATH, 0, 0, tiled=True)


def shards(states, itm_flags, terminal, strike, date_index):
    dates, factors, paths = states.shape
    size = lax.axis_size(PATH)
    sds = jax.ShapeDtypeStruct
    terminal = terminal.reshape(1, paths)
    date_index = date_index.reshape(1, paths)
    vmem = pltpu.VMEM
    limit = pltpu.CompilerParams(vmem_limit_bytes=24 << 20)
    stats = pl.pallas_call(
        stats_kernel,
        grid=(2,),
        in_specs=[
            pl.BlockSpec((dates // 2, factors, paths), lambda i: (i, 0, 0)),
            spec((dates, paths)),
        ],
        out_shape=vmem((size, 8, 128), f32),
        out_specs=WHOLE,
        scratch_shapes=[pltpu.VMEM((24, 128), f32)],
        compiler_params=limit,
        name="stats",
    )(pltpu.with_memory_space_constraint(states, pltpu.HBM), pltpu.with_memory_space_constraint(itm_flags, pltpu.HBM))
    stats = exchange(stats)
    place = jnp.full((1, 256), lax.axis_index(PATH), jnp.int32)
    exercise, discount = pl.pallas_call(
        swap_kernel,
        in_specs=[pl.BlockSpec(memory_space=pltpu.SMEM), WHOLE],
        out_specs=[WHOLE, WHOLE],
        out_shape=[vmem((dates, paths), f32), vmem((dates, paths), f32)],
        scratch_shapes=[pltpu.VMEM((factors, paths), f32)],
        compiler_params=limit,
        name="swap",
    )(strike, states)

    tiles = paths // 128
    discount, place = lax.optimization_barrier((discount, place))
    slots, value = pl.pallas_call(
        gram_kernel,
        grid=(dates,),
        in_specs=[WHOLE] * 5,
        out_specs=[WHOLE] * 2,
        out_shape=[vmem((size, SLOT, 256), f32), vmem((1, paths), f32)],
        scratch_shapes=[
            pltpu.VMEM((tiles, ROWS, 128), f32),
            pltpu.VMEM((tiles, 32, 128), f32),
            pltpu.VMEM((256, 256), f32),
            pltpu.VMEM((1, 256), f32),
            pltpu.VMEM((dates, factors, 128), f32),
            pltpu.VMEM((dates, factors, 128), f32),
        ],
        compiler_params=limit,
        name="gram",
    )(near(stats), near(states), near(itm_flags), near(discount), near(terminal))
    phi = pl.pallas_call(
        basis_kernel,
        grid=(dates,),
        in_specs=[
            spec((size, 8, 128)),
            pl.BlockSpec((None, factors, paths), lambda i: (dates - 1 - i, 0, 0)),
            spec((dates, paths)),
        ],
        out_specs=[pl.BlockSpec(memory_space=pltpu.HBM)] * dates,
        out_shape=[pltpu.HBM((tiles, ROWS, 128), f32)] * dates,
        scratch_shapes=[
            pltpu.VMEM((2, tiles, ROWS, 128), f32),
            pltpu.VMEM((tiles, 32, 128), f32),
            pltpu.SemaphoreType.DMA((2,)),
        ],
        compiler_params=limit,
        name="basis",
    )(stats, states, itm_flags)
    slots = exchange(slots)
    def invert(*refs):
        inverse_kernel(dates, *refs)

    inverse, rest, received = pl.pallas_call(
        invert,
        grid=(1,),
        in_specs=[WHOLE, WHOLE],
        out_specs=[spec((size, SENT, 256)), WHOLE, WHOLE],
        out_shape=[
            pltpu.HBM((size, SENT, 256), f32),
            vmem((SLOT - SENT, 256), f32),
            vmem((1, 1, 256), f32),
        ],
        scratch_shapes=[pltpu.VMEM((256, 256), f32)],
        compiler_params=limit,
        name="inverse",
    )(near(place), near(slots))
    inverse = exchange(inverse)
    pieces = pl.pallas_call(
        pieces_kernel,
        grid=(1,),
        in_specs=[WHOLE],
        out_specs=[spec((size, 1, WIDE))] * PIECES,
        out_shape=[pltpu.HBM((size, 1, WIDE), f32)] * PIECES,
        compiler_params=limit,
        name="pieces",
    )(near(rest))
    paired = 2 * dates - size

    def unfold_pairs(*refs):
        unfold_pairs_kernel(paired, dates, *refs)

    first_inverse = pl.pallas_call(
        unfold_pairs,
        grid=(1,),
        in_specs=[spec((size, SENT, 256))],
        out_specs=WHOLE,
        out_shape=vmem((dates - paired, ROWS, 256), f32),
        compiler_params=limit,
        name="unfold_pairs",
    )(inverse)
    other_inverse = None
    carried = []
    coefs = None
    for date in range(dates - 1, -1, -1):
        if date == paired - 1:
            other_inverse = pl.pallas_call(
                unfold_pieces_kernel,
                grid=(1,),
                in_specs=[spec((paired, SENT, 256))] + [WHOLE] * PIECES,
                out_specs=WHOLE,
                out_shape=vmem((paired, ROWS, 256), f32),
                scratch_shapes=[pltpu.VMEM((paired, SLOT, 256), f32)],
                compiler_params=limit,
                name="unfold_pieces",
            )(inverse, *(near(x) for x in carried))
        first_date = paired if date >= paired else 0
        args = [first_inverse if date >= paired else other_inverse, received, phi[date], exercise, itm_flags, date_index, value, discount]
        if date:
            args.append(phi[date - 1])
        if date < dates - 1:
            args.append(coefs)
        carries = len(carried) < PIECES
        aliases = {}
        if carries:
            aliases = {len(args): 2}
            args.append(pieces[len(carried)])

        def kernel(*refs, date=date, first_date=first_date):
            chain_kernel(date, dates, first_date, *refs)

        value, coefs, send = pl.pallas_call(
            kernel,
            in_specs=[WHOLE] * len(args),
            out_specs=[WHOLE] * 3,
            out_shape=[
                vmem((1, paths), f32),
                vmem((ROWS, 128), f32),
                vmem((size, 1, WIDE if carries else 256), f32),
            ]
            if date
            else [sds((1, paths), f32), sds((128, 256), f32), sds((size, 1, 128), f32)],
            input_output_aliases=aliases,
            compiler_params=limit,
            name="chain",
        )(*(near(x) for x in args))
        received = exchange(send)
        if carries:
            carried.append(received)
    book_price = jnp.sum(received[:, 0, 0:1], axis=0) / (paths * size)
    basis = 1 + factors + factors * (factors + 1) // 2
    coefficients = coefs[0:dates, 0:basis]
    return (value.reshape(paths), book_price, coefficients)


def solution(mesh):
    split = Mesh(mesh.devices.reshape(mesh.shape["book"], 4, 4), ("book", "path_0", "path_1"))
    return jax.shard_map(
        shards,
        mesh=split,
        in_specs=(
            P(None, None, BOOK_PATH),
            P(None, BOOK_PATH),
            P(BOOK_PATH),
            P("book"),
            P(BOOK_PATH),
        ),
        out_specs=(P(BOOK_PATH), P("book"), P("book", None)),
        check_vma=False,
    )
```

```python
import jax
import jax.numpy as jnp
from jax import lax
from jax.experimental import pallas as pl
from jax.experimental.pallas import tpu as pltpu
from jax.sharding import Mesh
from jax.sharding import PartitionSpec as P

PATH = ("path_0", "path_1")
BOOK_PATH = ("book", "path_0", "path_1")
ridge_weight = 0.05
temper_scale = 0.5
highest = lax.Precision.HIGHEST
f32 = jnp.float32
bf16 = jnp.bfloat16
NT = (((1,), (1,)), ((), ()))
TN = (((0,), (0,)), ((), ()))
ROWS = 240
HALF = 128
REST = 104
SLOT = 112
SENT = 64
PIECES = 6
WIDE = 256 * 9
BLOCK = 16


def spec(shape, index=None):
    if index is None:
        index = (0,) * len(shape)
    return pl.BlockSpec(shape, lambda *_: index)


WHOLE = pl.BlockSpec(memory_space=pltpu.VMEM)


def near(x):
    return pltpu.with_memory_space_constraint(x, pltpu.VMEM)


def lanes_of(shape):
    return lax.broadcasted_iota(jnp.int32, shape, 1)


def rows_of(shape):
    return lax.broadcasted_iota(jnp.int32, shape, 0)


def stats_kernel(z_ref, m_ref, out_ref, sum_ref):
    step = pl.program_id(0)
    dates, factors, _ = z_ref.shape
    lane = lanes_of((factors, 128))

    @pl.when(step == 0)
    def _():
        sum_ref[...] = jnp.zeros_like(sum_ref)

    packed = sum_ref[0:factors, :]
    for i in range(dates):
        d = step * dates + i
        z = z_ref[i]
        m = m_ref[pl.ds(d, 1), :].astype(f32)
        mz = z * m
        packed = jnp.where(lane == 3 * d, jnp.sum(mz, axis=1, keepdims=True), packed)
        packed = jnp.where(lane == 3 * d + 1, jnp.sum(mz * z, axis=1, keepdims=True), packed)
        packed = jnp.where(lane == 3 * d + 2, jnp.sum(m, axis=1, keepdims=True), packed)
    sum_ref[0:factors, :] = packed
    groups = sum_ref[0:8] + pltpu.roll(sum_ref[8:16], 32, 1) + pltpu.roll(sum_ref[16:24], 64, 1)
    for i in range(out_ref.shape[0]):
        out_ref[i] = groups


def swap_kernel(strike_ref, z_ref, ex_ref, disc_ref, fac_ref):
    dates, factors, _ = z_ref.shape
    for d in range(dates):
        fac_ref[...] = 1.0 / (1.0 + 0.25 * (0.03 * jnp.exp(0.25 * z_ref[d])))
        first = fac_ref[0:1, :]
        disc = first
        total = first
        for j in range(1, factors):
            disc = disc * fac_ref[j : j + 1, :]
            total = total + disc
        disc_ref[d : d + 1, :] = first
        ex_ref[d : d + 1, :] = 100.0 * ((1.0 - disc) - strike_ref[0] * (0.25 * total))


def rhs_row(phi_ref, weights):
    acc = jnp.zeros((ROWS, 128), f32)
    for c in range(0, weights.shape[1], 128):
        acc = acc + phi_ref[c // 128] * weights[:, c : c + 128]
    row = lax.dot_general(
        jnp.ones((8, 128), f32), acc, NT, precision=highest, preferred_element_type=f32
    )
    return jnp.concatenate([row, jnp.zeros((8, 256 - ROWS), f32)], axis=1)


def column(stats, i):
    return jnp.sum(jnp.where(lanes_of(stats.shape) == i, stats, 0.0), axis=1, keepdims=True)


def moments(stats_ref, d, factors):
    stats = stats_ref[0]
    for i in range(1, stats_ref.shape[0]):
        stats = stats + stats_ref[i]
    stats = jnp.concatenate([stats, pltpu.roll(stats, 96, 1), pltpu.roll(stats, 64, 1)], axis=0)[0:factors]
    count = column(stats, 3 * d + 2)
    mean = column(stats, 3 * d) / count
    return mean, 1.0 / jnp.sqrt(column(stats, 3 * d + 1) / count - mean * mean + 1e-05)


def fill_basis(phi_ref, x_ref, z, m, mean, inverse):
    factors = z.shape[0]
    x_ref[0:factors, :] = (z - mean) * inverse * m
    phi_ref[0:1, :] = m
    phi_ref[1 : 1 + factors, :] = x_ref[0:factors, :]
    offset = 1 + factors
    for j in range(factors):
        left = jnp.broadcast_to(x_ref[j : j + 1, :], (8, 128))
        for k in range(0, factors - j, 8):
            phi_ref[offset + k : offset + k + 8, :] = left * x_ref[j + k : j + k + 8, :]
        offset += factors - j
    phi_ref[offset : offset + 8, :] = jnp.zeros((8, 128), f32)
    phi_ref[ROWS - 8 : ROWS, :] = jnp.zeros((8, 128), f32)


def basis_kernel(stats_ref, z_ref, m_ref, *refs):
    *phi_refs, phi_two_ref, x_ref, sems = refs
    step = pl.program_id(0)
    dates, paths = m_ref.shape
    d = dates - 1 - step
    side = step % 2

    def copy_of(half, date):
        return pltpu.make_async_copy(phi_two_ref.at[half], phi_refs[date], sems.at[half])

    @pl.when(step >= 2)
    def _():
        copy_of(side, 0).wait()

    mean, inverse = moments(stats_ref, d, z_ref.shape[0])
    m = m_ref[pl.ds(d, 1), :].astype(f32)
    for t in range(paths // 128):
        at = slice(t * 128, (t + 1) * 128)
        fill_basis(phi_two_ref.at[side, t], x_ref.at[t], z_ref[:, at], m[:, at], mean, inverse)
    for date in range(dates):

        @pl.when(d == date)
        def _(date=date):
            copy_of(side, date).start()

    @pl.when(step == dates - 1)
    def _():
        for half in range(2):
            copy_of(half, 0).wait()


def gram_kernel(stats_ref, z_all_ref, m_ref, disc_ref, term_ref, slots_ref, v_ref, *scratch):
    phi_ref, x_ref, gram_ref, cross_ref, rhs_ref, mean_ref, inverse_ref = scratch
    step = pl.program_id(0)
    dates, factors, paths = z_all_ref.shape
    d = dates - 1 - step

    @pl.when(step == 0)
    def _():
        x_ref[...] = jnp.zeros_like(x_ref)
        gram_ref[...] = jnp.zeros_like(gram_ref)
        cross_ref[...] = jnp.zeros_like(cross_ref)
        v_ref[...] = term_ref[...] * disc_ref[dates - 1 : dates, :]
        for date in range(dates):
            mean, inverse = moments(stats_ref, date, factors)
            mean_ref[date] = jnp.broadcast_to(mean, (factors, 128))
            inverse_ref[date] = jnp.broadcast_to(inverse, (factors, 128))

    def fold(date, first):
        cross = cross_ref[...]
        gram = gram_ref[...] + cross + cross.T
        row, lane = rows_of((HALF, HALF)), lanes_of((HALF, HALF))
        beside = jnp.where(lane < REST, gram[0:HALF, HALF:], 0.0)
        under = jnp.where((row < REST) & (lane < REST), gram[HALF:, HALF:], 0.0)
        rhs = jnp.sum(gram[ROWS : ROWS + 3, :], axis=0, keepdims=True)
        rhs = jnp.where(first, rhs, rhs_ref[...])
        rhs_ref[...] = rhs
        packed = folded(gram[0:HALF, 0:HALF], beside, under, rhs)
        slots_ref[date] = packed
        again = 2 * dates - 1 - date
        slots_ref[jnp.where(again < slots_ref.shape[0], again, date)] = packed

    fold(d + 1, step == 1)
    flags = m_ref[pl.ds(d, 1), :].astype(f32)
    values = jnp.where(step == 0, v_ref[...], 0.0)
    mean, inverse = mean_ref[d], inverse_ref[d]
    total = None
    for pair in range(0, paths // 128, 2):
        hi, lo = [], []
        for t in (pair, pair + 1):
            at = slice(t * 128, (t + 1) * 128)
            fill_basis(phi_ref.at[t], x_ref.at[t], z_all_ref[d, :, at], flags[:, at], mean, inverse)
            phi = phi_ref[t]
            high = phi.astype(bf16)
            low = (phi - high.astype(f32)).astype(bf16)
            value = values[:, at]
            one = value.astype(bf16).astype(f32)
            two = (value - one).astype(bf16).astype(f32)
            three = value - one - two
            row = rows_of((256 - ROWS, 128))
            under = jnp.where(row == 0, one, jnp.where(row == 1, two, jnp.where(row == 2, three, 0.0)))
            hi.append(jnp.concatenate([high, under.astype(bf16)], axis=0))
            lo.append(jnp.concatenate([low, jnp.zeros((256 - ROWS, 128), bf16)], axis=0))
        hi = jnp.concatenate(hi, axis=1)
        lo = jnp.concatenate(lo, axis=1)
        both = lax.dot_general(
            jnp.concatenate([hi, lo], axis=0), hi, NT, preferred_element_type=f32
        )
        total = both if total is None else total + both
    gram_ref[...] = total[0:256]
    cross_ref[...] = total[256:]

    @pl.when(step == dates - 1)
    def _():
        fold(0, False)


def folded(first, beside, last, rhs=None):
    row, lane = rows_of((HALF, HALF)), lanes_of((HALF, HALF))
    left = jnp.where(row <= lane, first, last)
    low_lane = lanes_of((8, HALF))
    low = left[REST:SLOT]
    low = jnp.where(low_lane < 16, pltpu.roll(first[SLOT : SLOT + 8], 16, 1), low)
    low = jnp.where((low_lane >= 16) & (low_lane < 32), pltpu.roll(first[SLOT + 8 :], 32, 1), low)
    if rhs is not None:
        low_row = rows_of((8, HALF))
        for i in range(4):
            piece = pltpu.roll(jnp.broadcast_to(rhs, (8, 256)), (32 - 72 * i) % 256, 1)[:, 0:HALF]
            low = jnp.where((low_row == i) & (low_lane >= 32) & (low_lane < REST), piece, low)
    left = jnp.concatenate([left[0:REST], low], axis=0)
    diagonal = jnp.sum(jnp.where(row == lane, last, 0.0), axis=1, keepdims=True)
    right = jnp.where(lane < REST, beside, pltpu.roll(beside.T, HALF - 8, 1))
    right = jnp.where(lane == 120, diagonal, right)[0:SLOT]
    return jnp.concatenate([left, right], axis=1)


def unfolded(packed):
    row, lane = rows_of((HALF, HALF)), lanes_of((HALF, HALF))
    none = jnp.zeros((HALF - SLOT, HALF), f32)
    left = jnp.concatenate([packed[:, 0:HALF], none], axis=0)
    right = jnp.concatenate([packed[:, HALF:], none], axis=0)
    low = left[REST:SLOT]
    corner = jnp.concatenate(
        [left[0:SLOT], pltpu.roll(low, HALF - 16, 1), pltpu.roll(low, HALF - 32, 1)], axis=0
    )
    turned = left.T
    first = jnp.where(row <= lane, left, turned)
    first = jnp.where((row >= SLOT) & (lane >= SLOT), corner, first)
    diagonal = jnp.sum(jnp.where(lane == 120, right, 0.0), axis=1, keepdims=True)
    last = jnp.where(row > lane, left, turned)
    last = jnp.where(row == lane, diagonal, last)
    last = jnp.where((row < REST) & (lane < REST), last, 0.0)
    beside = jnp.where(row < SLOT, right, pltpu.roll(right, 8, 1).T)
    beside = jnp.where(lane < REST, beside, 0.0)
    return first, beside, last


def unfolded_row(low):
    lane = lanes_of((1, 256))
    wide = jnp.concatenate([low, jnp.zeros((8, HALF), f32)], axis=1)
    total = jnp.zeros((1, 256), f32)
    for i in range(4):
        piece = pltpu.roll(wide, (72 * i - 32) % 256, 1)[i : i + 1]
        total = jnp.where((lane >= 72 * i) & (lane < min(72 * i + 72, 231)), piece, total)
    return total


def inverse_kernel(dates, place_ref, parts_ref, out_ref, rest_ref, rhs_ref, a_ref):
    basis = 231
    packed = parts_ref[0]
    for i in range(1, parts_ref.shape[0]):
        packed = packed + parts_ref[i]
    rhs_ref[0] = unfolded_row(packed[REST:SLOT, 0:HALF])
    first, beside, last = unfolded(packed)
    a_ref[0:HALF, 0:HALF] = first
    a_ref[0:HALF, HALF:] = beside
    a_ref[HALF:, 0:HALF] = beside.T
    a_ref[HALF:, HALF:] = last
    count = packed[0:1, 0:1]
    row, lane = rows_of((256, 256)), lanes_of((256, 256))
    added = jnp.where(row < basis, ridge_weight * count, 1.0)
    a_ref[...] = a_ref[...] + jnp.where(row == lane, added, 0.0)
    lane_a = lanes_of((BLOCK, 128))
    lane_b = lane_a + 128
    row_a = rows_of((BLOCK, 128))
    lane_r = lanes_of((BLOCK, 256))

    def split(x):
        one = x.astype(bf16)
        rest = x - one.astype(f32)
        two = rest.astype(bf16)
        return one, two, (rest - two.astype(f32)).astype(bf16)

    def sweep(i, carry):
        start = pl.multiple_of(i * BLOCK, BLOCK)
        panel = a_ref[pl.ds(start, BLOCK), :]
        ra, rb = panel[:, 0:128], panel[:, 128:]
        cols = []
        for c in range(BLOCK):
            both = jnp.where(lane_a == start + c, ra, 0.0) + jnp.where(lane_b == start + c, rb, 0.0)
            cols.append(jnp.broadcast_to(jnp.sum(both, axis=1, keepdims=True), (BLOCK, 128)))
        for k in range(BLOCK):
            pivot = 1.0 / cols[k][k : k + 1, :]
            here = row_a == k
            unit = jnp.where(here, 1.0, 0.0)
            ra = jnp.where(lane_a == start + k, unit, ra)
            rb = jnp.where(lane_b == start + k, unit, rb)
            row_k = ra[k : k + 1, :] * pivot
            ra = jnp.where(here, row_k, ra - cols[k] * row_k)
            row_k = rb[k : k + 1, :] * pivot
            rb = jnp.where(here, row_k, rb - cols[k] * row_k)
            for c in range(k + 1, BLOCK):
                f = cols[c][k : k + 1, :] * pivot
                cols[c] = jnp.where(here, f, cols[c] - cols[k] * f)
        inside = (lane_r >= start) & (lane_r < start + BLOCK)
        w = jnp.concatenate([ra, rb], axis=1)
        w = jnp.where(inside, -w, w)
        r1, r2, r3 = split(panel)
        w1, w2, w3 = split(w)
        left = jnp.concatenate([r1, r1, r2, r2, r1, r3], axis=0)
        right = jnp.concatenate([w1, w2, w1, w2, w3, w1], axis=0)
        change = lax.dot_general(left, right, TN, preferred_element_type=f32)
        within = (lane >= start) & (lane < start + BLOCK)
        a_ref[...] = jnp.where(within, 0.0, a_ref[...]) - change
        a_ref[pl.ds(start, BLOCK), :] = w
        return carry

    lax.fori_loop(0, ROWS // BLOCK, sweep, 0)
    result = -a_ref[...]
    packed = folded(result[0:HALF, 0:HALF], result[0:HALF, HALF:], result[HALF:, HALF:])
    own = jnp.broadcast_to(place_ref[...] < dates, (SENT, 256))
    sent = jnp.where(own, packed[0:SENT], packed[SLOT - SENT :])
    for i in range(out_ref.shape[0]):
        out_ref[i] = sent
    rest_ref[...] = packed[SENT:SLOT]


def pieces_kernel(rest_ref, *out_refs):
    for p, out_ref in enumerate(out_refs):
        for i in range(out_ref.shape[0]):
            out_ref[i, :, 0:256] = jnp.zeros((1, 256), f32)
            for r in range(8):
                row = 8 * p + r
                out_ref[i, :, 256 * (1 + r) : 256 * (2 + r)] = rest_ref[row : row + 1, :]


def unfold_pairs_kernel(first_date, dates, parts_ref, *refs):
    *far_refs, out_ref, near_a_ref, near_b_ref, sems = refs
    copies = [
        pltpu.make_async_copy(far, beside, sems.at[i])
        for i, (far, beside) in enumerate(zip(far_refs, (near_a_ref, near_b_ref)))
    ]
    for copy in copies:
        copy.start()
    for i in range(out_ref.shape[0]):
        date = first_date + i
        rest = parts_ref[2 * dates - 1 - date]
        write_unfolded(jnp.concatenate([parts_ref[date], rest[2 * SENT - SLOT :]], axis=0), out_ref.at[i])
    for copy in copies:
        copy.wait()


def unfold_pieces_kernel(parts_ref, *refs):
    *piece_refs, out_ref, packed_ref = refs
    for i in range(out_ref.shape[0]):
        packed_ref[i, 0:SENT, :] = parts_ref[i]
        for p, piece_ref in enumerate(piece_refs):
            for r in range(8):
                row = SENT + 8 * p + r
                packed_ref[i, row : row + 1, :] = piece_ref[i, :, 256 * (1 + r) : 256 * (2 + r)]
        write_unfolded(packed_ref[i], out_ref.at[i])


def write_unfolded(packed, out_ref):
    first, beside, last = unfolded(packed)
    out_ref[0:HALF, 0:HALF] = first
    out_ref[0:HALF, HALF:] = beside
    out_ref[HALF:, 0:HALF] = beside.T[0 : ROWS - HALF, :]
    out_ref[HALF:, HALF:] = last[0 : ROWS - HALF, :]


def chain_kernel(date, dates, first_date, *refs):
    inv_ref, parts_ref, phi_ref, ex_ref, m_ref, index_ref, v_ref, disc_ref = refs[:8]
    refs = refs[8:]
    if date:
        next_ref = refs[0]
        refs = refs[1:]
    if date == dates - 1:
        coefs = jnp.zeros((ROWS, 128), f32)
    else:
        coefs = refs[0][...]
        refs = refs[1:]
    if len(refs) == 4:
        refs = refs[1:]
    rhs = parts_ref[0, :, 0:256]
    for i in range(1, parts_ref.shape[0]):
        rhs = rhs + parts_ref[i, :, 0:256]
    product = inv_ref[date - first_date] * rhs
    coef = jnp.sum(product[:, 0:128] + product[:, 128:], axis=1, keepdims=True)
    coef = jnp.broadcast_to(coef, (ROWS, 128))
    out_ref, coef_ref, send_ref = refs
    continuation = []
    for c in range(0, v_ref.shape[1], 128):
        continuation.append(jnp.sum(coef * phi_ref[c // 128], axis=0, keepdims=True))
    continuation = jnp.concatenate(continuation, axis=1)
    exercise = ex_ref[date : date + 1, :]
    opened = jnp.where(index_ref[...] <= date, m_ref[date : date + 1, :].astype(f32), 0.0)
    weights = jax.nn.sigmoid((exercise - continuation) / temper_scale) * opened
    value = v_ref[...]
    value = value + weights * (exercise - value)
    if date:
        value = value * disc_ref[date - 1 : date, :]
        row = rhs_row(next_ref, value)
        for i in range(send_ref.shape[0]):
            send_ref[i, :, 0:256] = row[0:1, :]
    else:
        total = jnp.broadcast_to(jnp.sum(value, axis=1, keepdims=True), (1, 128))
        for i in range(send_ref.shape[0]):
            send_ref[i] = total
    out_ref[...] = value
    coefs = jnp.where(lanes_of((ROWS, 128)) == date, coef, coefs)
    if date:
        coef_ref[...] = coefs
    else:
        for c in range(0, ROWS, 128):
            coef_ref[:, c : c + 128] = coefs[0:128, :].T if c == 0 else jnp.concatenate(
                [coefs[c:, :], jnp.zeros((128 - (ROWS - c), 128), f32)], axis=0
            ).T


def exchange(slots):
    return lax.all_to_all(slots, PATH, 0, 0, tiled=True)


def shards(states, itm_flags, terminal, strike, date_index):
    dates, factors, paths = states.shape
    size = lax.axis_size(PATH)
    sds = jax.ShapeDtypeStruct
    terminal = terminal.reshape(1, paths)
    date_index = date_index.reshape(1, paths)
    vmem = pltpu.VMEM
    limit = pltpu.CompilerParams(vmem_limit_bytes=24 << 20)
    stats = pl.pallas_call(
        stats_kernel,
        grid=(2,),
        in_specs=[
            pl.BlockSpec((dates // 2, factors, paths), lambda i: (i, 0, 0)),
            spec((dates, paths)),
        ],
        out_shape=vmem((size, 8, 128), f32),
        out_specs=WHOLE,
        scratch_shapes=[pltpu.VMEM((24, 128), f32)],
        compiler_params=limit,
        name="stats",
    )(pltpu.with_memory_space_constraint(states, pltpu.HBM), pltpu.with_memory_space_constraint(itm_flags, pltpu.HBM))
    stats = exchange(stats)
    place = jnp.full((1, 256), lax.axis_index(PATH), jnp.int32)
    exercise, discount = pl.pallas_call(
        swap_kernel,
        in_specs=[pl.BlockSpec(memory_space=pltpu.SMEM), WHOLE],
        out_specs=[WHOLE, WHOLE],
        out_shape=[vmem((dates, paths), f32), vmem((dates, paths), f32)],
        scratch_shapes=[pltpu.VMEM((factors, paths), f32)],
        compiler_params=limit,
        name="swap",
    )(strike, states)

    tiles = paths // 128
    discount, place = lax.optimization_barrier((discount, place))
    slots, value = pl.pallas_call(
        gram_kernel,
        grid=(dates,),
        in_specs=[WHOLE] * 5,
        out_specs=[WHOLE] * 2,
        out_shape=[vmem((size, SLOT, 256), f32), vmem((1, paths), f32)],
        scratch_shapes=[
            pltpu.VMEM((tiles, ROWS, 128), f32),
            pltpu.VMEM((tiles, 32, 128), f32),
            pltpu.VMEM((256, 256), f32),
            pltpu.VMEM((256, 256), f32),
            pltpu.VMEM((1, 256), f32),
            pltpu.VMEM((dates, factors, 128), f32),
            pltpu.VMEM((dates, factors, 128), f32),
        ],
        compiler_params=limit,
        name="gram",
    )(near(stats), near(states), near(itm_flags), near(discount), near(terminal))
    phi = pl.pallas_call(
        basis_kernel,
        grid=(dates,),
        in_specs=[
            spec((size, 8, 128)),
            pl.BlockSpec((None, factors, paths), lambda i: (dates - 1 - i, 0, 0)),
            spec((dates, paths)),
        ],
        out_specs=[pl.BlockSpec(memory_space=pltpu.HBM)] * dates,
        out_shape=[pltpu.HBM((tiles, ROWS, 128), f32)] * dates,
        scratch_shapes=[
            pltpu.VMEM((2, tiles, ROWS, 128), f32),
            pltpu.VMEM((tiles, 32, 128), f32),
            pltpu.SemaphoreType.DMA((2,)),
        ],
        compiler_params=limit,
        name="basis",
    )(stats, states, itm_flags)
    slots = exchange(slots)
    def invert(*refs):
        inverse_kernel(dates, *refs)

    inverse, rest, received = pl.pallas_call(
        invert,
        grid=(1,),
        in_specs=[WHOLE, WHOLE],
        out_specs=[spec((size, SENT, 256)), WHOLE, WHOLE],
        out_shape=[
            pltpu.HBM((size, SENT, 256), f32),
            vmem((SLOT - SENT, 256), f32),
            vmem((1, 1, 256), f32),
        ],
        scratch_shapes=[pltpu.VMEM((256, 256), f32)],
        compiler_params=limit,
        name="inverse",
    )(near(place), near(slots))
    inverse = exchange(inverse)
    pieces = pl.pallas_call(
        pieces_kernel,
        grid=(1,),
        in_specs=[WHOLE],
        out_specs=[spec((size, 1, WIDE))] * PIECES,
        out_shape=[pltpu.HBM((size, 1, WIDE), f32)] * PIECES,
        compiler_params=limit,
        name="pieces",
    )(near(rest))
    paired = 2 * dates - size

    def unfold_pairs(*refs):
        unfold_pairs_kernel(paired, dates, *refs)

    first_inverse, *near_phi = pl.pallas_call(
        unfold_pairs,
        grid=(1,),
        in_specs=[spec((size, SENT, 256))] + [pl.BlockSpec(memory_space=pltpu.HBM)] * 2,
        out_specs=[WHOLE] * 3,
        out_shape=[vmem((dates - paired, ROWS, 256), f32)] + [vmem((tiles, ROWS, 128), f32)] * 2,
        scratch_shapes=[pltpu.SemaphoreType.DMA((2,))],
        compiler_params=limit,
        name="unfold_pairs",
    )(inverse, *(pltpu.with_memory_space_constraint(phi[d], pltpu.HBM) for d in (dates - 1, dates - 2)))
    phi = [*phi[: dates - 2], *near_phi[::-1]]
    other_inverse = None
    carried = []
    coefs = None
    for date in range(dates - 1, -1, -1):
        if date == paired - 1:
            other_inverse = pl.pallas_call(
                unfold_pieces_kernel,
                grid=(1,),
                in_specs=[spec((paired, SENT, 256))] + [WHOLE] * PIECES,
                out_specs=WHOLE,
                out_shape=vmem((paired, ROWS, 256), f32),
                scratch_shapes=[pltpu.VMEM((paired, SLOT, 256), f32)],
                compiler_params=limit,
                name="unfold_pieces",
            )(inverse, *(near(x) for x in carried))
        first_date = paired if date >= paired else 0
        args = [first_inverse if date >= paired else other_inverse, received, phi[date], exercise, itm_flags, date_index, value, discount]
        if date:
            args.append(phi[date - 1])
        if date < dates - 1:
            args.append(coefs)
        carries = len(carried) < PIECES
        aliases = {}
        if carries:
            aliases = {len(args): 2}
            args.append(pieces[len(carried)])

        def kernel(*refs, date=date, first_date=first_date):
            chain_kernel(date, dates, first_date, *refs)

        value, coefs, send = pl.pallas_call(
            kernel,
            in_specs=[WHOLE] * len(args),
            out_specs=[WHOLE] * 3,
            out_shape=[
                vmem((1, paths), f32),
                vmem((ROWS, 128), f32),
                vmem((size, 1, WIDE if carries else 256), f32),
            ]
            if date
            else [sds((1, paths), f32), sds((128, 256), f32), sds((size, 1, 128), f32)],
            input_output_aliases=aliases,
            compiler_params=limit,
            name="chain",
        )(*(near(x) for x in args))
        received = exchange(send)
        if carries:
            carried.append(received)
    book_price = jnp.sum(received[:, 0, 0:1], axis=0) / (paths * size)
    basis = 1 + factors + factors * (factors + 1) // 2
    coefficients = coefs[0:dates, 0:basis]
    return (value.reshape(paths), book_price, coefficients)


def solution(mesh):
    split = Mesh(mesh.devices.reshape(mesh.shape["book"], 4, 4), ("book", "path_0", "path_1"))
    return jax.shard_map(
        shards,
        mesh=split,
        in_specs=(
            P(None, None, BOOK_PATH),
            P(None, BOOK_PATH),
            P(BOOK_PATH),
            P("book"),
            P(BOOK_PATH),
        ),
        out_specs=(P(BOOK_PATH), P("book"), P("book", None)),
        check_vma=False,
    )
```

```python
import jax
import jax.numpy as jnp
from jax import lax
from jax.experimental import pallas as pl
from jax.experimental.pallas import tpu as pltpu
from jax.sharding import Mesh
from jax.sharding import PartitionSpec as P

PATH = ("path_0", "path_1")
BOOK_PATH = ("book", "path_0", "path_1")
ridge_weight = 0.05
temper_scale = 0.5
f32 = jnp.float32
bf16 = jnp.bfloat16
NT = (((1,), (1,)), ((), ()))
TN = (((0,), (0,)), ((), ()))
ROWS = 240
HALF = 128
REST = 104
SLOT = 112
SENT = 64
PIECES = 6
WIDE = 256 * 9
BLOCK = 16


def spec(shape, index=None):
    if index is None:
        index = (0,) * len(shape)
    return pl.BlockSpec(shape, lambda *_: index)


WHOLE = pl.BlockSpec(memory_space=pltpu.VMEM)


def near(x):
    return pltpu.with_memory_space_constraint(x, pltpu.VMEM)


def lanes_of(shape):
    return lax.broadcasted_iota(jnp.int32, shape, 1)


def rows_of(shape):
    return lax.broadcasted_iota(jnp.int32, shape, 0)


def stats_kernel(z_ref, m_ref, out_ref, sum_ref):
    step = pl.program_id(0)
    dates, factors, _ = z_ref.shape
    lane = lanes_of((factors, 128))

    @pl.when(step == 0)
    def _():
        sum_ref[...] = jnp.zeros_like(sum_ref)

    packed = sum_ref[0:factors, :]
    for i in range(dates):
        d = step * dates + i
        z = z_ref[i]
        m = m_ref[pl.ds(d, 1), :].astype(f32)
        mz = z * m
        packed = jnp.where(lane == 3 * d, jnp.sum(mz, axis=1, keepdims=True), packed)
        packed = jnp.where(lane == 3 * d + 1, jnp.sum(mz * z, axis=1, keepdims=True), packed)
        packed = jnp.where(lane == 3 * d + 2, jnp.sum(m, axis=1, keepdims=True), packed)
    sum_ref[0:factors, :] = packed
    groups = sum_ref[0:8] + pltpu.roll(sum_ref[8:16], 32, 1) + pltpu.roll(sum_ref[16:24], 64, 1)
    for i in range(out_ref.shape[0]):
        out_ref[i] = groups


def swap_kernel(strike_ref, z_ref, ex_ref, disc_ref, fac_ref):
    dates, factors, _ = z_ref.shape
    for d in range(dates):
        fac_ref[...] = 1.0 / (1.0 + 0.25 * (0.03 * jnp.exp(0.25 * z_ref[d])))
        first = fac_ref[0:1, :]
        disc = first
        total = first
        for j in range(1, factors):
            disc = disc * fac_ref[j : j + 1, :]
            total = total + disc
        disc_ref[d : d + 1, :] = first
        ex_ref[d : d + 1, :] = 100.0 * ((1.0 - disc) - strike_ref[0] * (0.25 * total))


def split(x):
    one = x.astype(bf16)
    rest = x - one.astype(f32)
    two = rest.astype(bf16)
    return one, two, (rest - two.astype(f32)).astype(bf16)


def rhs_row(phi_ref, weights):
    acc = jnp.zeros((ROWS, 128), f32)
    for c in range(0, weights.shape[1], 128):
        acc = acc + phi_ref[c // 128] * weights[:, c : c + 128]
    ones = jnp.ones((16, 128), bf16)
    one, two, three = (lax.dot_general(ones, x, NT, preferred_element_type=f32) for x in split(acc))
    row = (one + two + three)[0:8]
    return jnp.concatenate([row, jnp.zeros((8, 256 - ROWS), f32)], axis=1)


def column(stats, i):
    return jnp.sum(jnp.where(lanes_of(stats.shape) == i, stats, 0.0), axis=1, keepdims=True)


def moments(stats_ref, d, factors):
    stats = stats_ref[0]
    for i in range(1, stats_ref.shape[0]):
        stats = stats + stats_ref[i]
    stats = jnp.concatenate([stats, pltpu.roll(stats, 96, 1), pltpu.roll(stats, 64, 1)], axis=0)[0:factors]
    count = column(stats, 3 * d + 2)
    mean = column(stats, 3 * d) / count
    return mean, 1.0 / jnp.sqrt(column(stats, 3 * d + 1) / count - mean * mean + 1e-05)


def fill_basis(phi_ref, x_ref, z, m, mean, inverse):
    factors = z.shape[0]
    x_ref[0:factors, :] = (z - mean) * inverse * m
    phi_ref[0:1, :] = m
    phi_ref[1 : 1 + factors, :] = x_ref[0:factors, :]
    offset = 1 + factors
    for j in range(factors):
        left = jnp.broadcast_to(x_ref[j : j + 1, :], (8, 128))
        for k in range(0, factors - j, 8):
            phi_ref[offset + k : offset + k + 8, :] = left * x_ref[j + k : j + k + 8, :]
        offset += factors - j
    phi_ref[offset : offset + 8, :] = jnp.zeros((8, 128), f32)
    phi_ref[ROWS - 8 : ROWS, :] = jnp.zeros((8, 128), f32)


def basis_kernel(stats_ref, z_ref, m_ref, *refs):
    *phi_refs, phi_two_ref, x_ref, sems = refs
    step = pl.program_id(0)
    dates, paths = m_ref.shape
    d = dates - 1 - step
    side = step % 2

    def copy_of(half, date):
        return pltpu.make_async_copy(phi_two_ref.at[half], phi_refs[date], sems.at[half])

    @pl.when(step >= 2)
    def _():
        copy_of(side, 0).wait()

    mean, inverse = moments(stats_ref, d, z_ref.shape[0])
    m = m_ref[pl.ds(d, 1), :].astype(f32)
    for t in range(paths // 128):
        at = slice(t * 128, (t + 1) * 128)
        fill_basis(phi_two_ref.at[side, t], x_ref.at[t], z_ref[:, at], m[:, at], mean, inverse)
    for date in range(dates):

        @pl.when(d == date)
        def _(date=date):
            copy_of(side, date).start()

    @pl.when(step == dates - 1)
    def _():
        for half in range(2):
            copy_of(half, 0).wait()


def gram_kernel(stats_ref, z_all_ref, m_ref, disc_ref, term_ref, slots_ref, v_ref, *scratch):
    phi_ref, x_ref, gram_ref, cross_ref, rhs_ref, mean_ref, inverse_ref = scratch
    step = pl.program_id(0)
    dates, factors, paths = z_all_ref.shape
    d = dates - 1 - step

    @pl.when(step == 0)
    def _():
        x_ref[...] = jnp.zeros_like(x_ref)
        gram_ref[...] = jnp.zeros_like(gram_ref)
        cross_ref[...] = jnp.zeros_like(cross_ref)
        v_ref[...] = term_ref[...] * disc_ref[dates - 1 : dates, :]
        for date in range(dates):
            mean, inverse = moments(stats_ref, date, factors)
            mean_ref[date] = jnp.broadcast_to(mean, (factors, 128))
            inverse_ref[date] = jnp.broadcast_to(inverse, (factors, 128))

    def fold(date, first):
        cross = cross_ref[...]
        gram = gram_ref[...] + cross + cross.T
        row, lane = rows_of((HALF, HALF)), lanes_of((HALF, HALF))
        beside = jnp.where(lane < REST, gram[0:HALF, HALF:], 0.0)
        under = jnp.where((row < REST) & (lane < REST), gram[HALF:, HALF:], 0.0)
        rhs = jnp.sum(gram[ROWS : ROWS + 3, :], axis=0, keepdims=True)
        rhs = jnp.where(first, rhs, rhs_ref[...])
        rhs_ref[...] = rhs
        packed = folded(gram[0:HALF, 0:HALF], beside, under, rhs)
        slots_ref[date] = packed
        again = 2 * dates - 1 - date
        slots_ref[jnp.where(again < slots_ref.shape[0], again, date)] = packed

    fold(d + 1, step == 1)
    flags = m_ref[pl.ds(d, 1), :].astype(f32)
    values = jnp.where(step == 0, v_ref[...], 0.0)
    mean, inverse = mean_ref[d], inverse_ref[d]
    total = None
    for pair in range(0, paths // 128, 2):
        hi, lo = [], []
        for t in (pair, pair + 1):
            at = slice(t * 128, (t + 1) * 128)
            fill_basis(phi_ref.at[t], x_ref.at[t], z_all_ref[d, :, at], flags[:, at], mean, inverse)
            phi = phi_ref[t]
            high = phi.astype(bf16)
            low = (phi - high.astype(f32)).astype(bf16)
            value = values[:, at]
            one = value.astype(bf16).astype(f32)
            two = (value - one).astype(bf16).astype(f32)
            three = value - one - two
            row = rows_of((256 - ROWS, 128))
            under = jnp.where(row == 0, one, jnp.where(row == 1, two, jnp.where(row == 2, three, 0.0)))
            hi.append(jnp.concatenate([high, under.astype(bf16)], axis=0))
            lo.append(jnp.concatenate([low, jnp.zeros((256 - ROWS, 128), bf16)], axis=0))
        hi = jnp.concatenate(hi, axis=1)
        lo = jnp.concatenate(lo, axis=1)
        both = lax.dot_general(
            jnp.concatenate([hi, lo], axis=0), hi, NT, preferred_element_type=f32
        )
        total = both if total is None else total + both
    gram_ref[...] = total[0:256]
    cross_ref[...] = total[256:]

    @pl.when(step == dates - 1)
    def _():
        fold(0, False)


def folded(first, beside, last, rhs=None):
    row, lane = rows_of((HALF, HALF)), lanes_of((HALF, HALF))
    left = jnp.where(row <= lane, first, last)
    low_lane = lanes_of((8, HALF))
    low = left[REST:SLOT]
    low = jnp.where(low_lane < 16, pltpu.roll(first[SLOT : SLOT + 8], 16, 1), low)
    low = jnp.where((low_lane >= 16) & (low_lane < 32), pltpu.roll(first[SLOT + 8 :], 32, 1), low)
    if rhs is not None:
        low_row = rows_of((8, HALF))
        for i in range(4):
            piece = pltpu.roll(jnp.broadcast_to(rhs, (8, 256)), (32 - 72 * i) % 256, 1)[:, 0:HALF]
            low = jnp.where((low_row == i) & (low_lane >= 32) & (low_lane < REST), piece, low)
    left = jnp.concatenate([left[0:REST], low], axis=0)
    diagonal = jnp.sum(jnp.where(row == lane, last, 0.0), axis=1, keepdims=True)
    right = jnp.where(lane < REST, beside, pltpu.roll(beside.T, HALF - 8, 1))
    right = jnp.where(lane == 120, diagonal, right)[0:SLOT]
    return jnp.concatenate([left, right], axis=1)


def unfolded(packed):
    row, lane = rows_of((HALF, HALF)), lanes_of((HALF, HALF))
    none = jnp.zeros((HALF - SLOT, HALF), f32)
    left = jnp.concatenate([packed[:, 0:HALF], none], axis=0)
    right = jnp.concatenate([packed[:, HALF:], none], axis=0)
    low = left[REST:SLOT]
    corner = jnp.concatenate(
        [left[0:SLOT], pltpu.roll(low, HALF - 16, 1), pltpu.roll(low, HALF - 32, 1)], axis=0
    )
    turned = left.T
    first = jnp.where(row <= lane, left, turned)
    first = jnp.where((row >= SLOT) & (lane >= SLOT), corner, first)
    diagonal = jnp.sum(jnp.where(lane == 120, right, 0.0), axis=1, keepdims=True)
    last = jnp.where(row > lane, left, turned)
    last = jnp.where(row == lane, diagonal, last)
    last = jnp.where((row < REST) & (lane < REST), last, 0.0)
    beside = jnp.where(row < SLOT, right, pltpu.roll(right, 8, 1).T)
    beside = jnp.where(lane < REST, beside, 0.0)
    return first, beside, last


def unfolded_row(low):
    lane = lanes_of((1, 256))
    wide = jnp.concatenate([low, jnp.zeros((8, HALF), f32)], axis=1)
    total = jnp.zeros((1, 256), f32)
    for i in range(4):
        piece = pltpu.roll(wide, (72 * i - 32) % 256, 1)[i : i + 1]
        total = jnp.where((lane >= 72 * i) & (lane < min(72 * i + 72, 231)), piece, total)
    return total


def inverse_kernel(dates, place_ref, parts_ref, out_ref, rest_ref, rhs_ref, a_ref):
    basis = 231
    packed = parts_ref[0]
    for i in range(1, parts_ref.shape[0]):
        packed = packed + parts_ref[i]
    rhs_ref[0] = unfolded_row(packed[REST:SLOT, 0:HALF])
    first, beside, last = unfolded(packed)
    a_ref[0:HALF, 0:HALF] = first
    a_ref[0:HALF, HALF:] = beside
    a_ref[HALF:, 0:HALF] = beside.T
    a_ref[HALF:, HALF:] = last
    count = packed[0:1, 0:1]
    row, lane = rows_of((256, 256)), lanes_of((256, 256))
    added = jnp.where(row < basis, ridge_weight * count, 1.0)
    a_ref[...] = a_ref[...] + jnp.where(row == lane, added, 0.0)
    lane_a = lanes_of((8, 128))
    lane_b = lane_a + 128
    row_a = rows_of((8, 128))
    lane_r = lanes_of((BLOCK, 256))

    def sweep(i, carry):
        start = pl.multiple_of(i * BLOCK, BLOCK)
        panel = a_ref[pl.ds(start, BLOCK), :]
        halves = [[panel[g : g + 8, h : h + 128] for g in range(0, BLOCK, 8)] for h in (0, 128)]
        cols = []
        for c in range(BLOCK):
            col = []
            for g in range(BLOCK // 8):
                both = jnp.where(lane_a == start + c, halves[0][g], 0.0)
                both = both + jnp.where(lane_b == start + c, halves[1][g], 0.0)
                col.append(jnp.broadcast_to(jnp.sum(both, axis=1, keepdims=True), (8, 128)))
            cols.append(col)
        for k in range(BLOCK):
            group, at = divmod(k, 8)
            here = row_a == at
            col = cols[k]
            pivot = 1.0 / col[group][at : at + 1, :]
            unit = jnp.where(here, 1.0, 0.0)

            def reduced(groups):
                scaled = groups[group][at : at + 1, :] * pivot
                out = [x - col[g] * scaled for g, x in enumerate(groups)]
                out[group] = jnp.where(here, scaled, out[group])
                return out

            for half, lane_h in zip(halves, (lane_a, lane_b)):
                is_k = lane_h == start + k
                for g in range(BLOCK // 8):
                    half[g] = jnp.where(is_k, unit if g == group else 0.0, half[g])
                half[:] = reduced(half)
            for c in range(k + 1, BLOCK):
                cols[c] = reduced(cols[c])
        inside = (lane_r >= start) & (lane_r < start + BLOCK)
        w = jnp.concatenate([jnp.concatenate(half, axis=0) for half in halves], axis=1)
        w = jnp.where(inside, -w, w)
        r1, r2, r3 = split(panel)
        w1, w2, w3 = split(w)
        left = jnp.concatenate([r1, r1, r2, r2, r1, r3], axis=0)
        right = jnp.concatenate([w1, w2, w1, w2, w3, w1], axis=0)
        change = lax.dot_general(left, right, TN, preferred_element_type=f32)
        within = (lane >= start) & (lane < start + BLOCK)
        a_ref[...] = jnp.where(within, 0.0, a_ref[...]) - change
        a_ref[pl.ds(start, BLOCK), :] = w
        return carry

    lax.fori_loop(0, ROWS // BLOCK, sweep, 0)
    result = -a_ref[...]
    packed = folded(result[0:HALF, 0:HALF], result[0:HALF, HALF:], result[HALF:, HALF:])
    own = jnp.broadcast_to(place_ref[...] < dates, (SENT, 256))
    sent = jnp.where(own, packed[0:SENT], packed[SLOT - SENT :])
    for i in range(out_ref.shape[0]):
        out_ref[i] = sent
    rest_ref[...] = packed[SENT:SLOT]


def pieces_kernel(rest_ref, *out_refs):
    for p, out_ref in enumerate(out_refs):
        for i in range(out_ref.shape[0]):
            out_ref[i, :, 0:256] = jnp.zeros((1, 256), f32)
            for r in range(8):
                row = 8 * p + r
                out_ref[i, :, 256 * (1 + r) : 256 * (2 + r)] = rest_ref[row : row + 1, :]


def unfold_pairs_kernel(first_date, dates, parts_ref, *refs):
    *far_refs, out_ref, near_a_ref, near_b_ref, sems = refs
    copies = [
        pltpu.make_async_copy(far, beside, sems.at[i])
        for i, (far, beside) in enumerate(zip(far_refs, (near_a_ref, near_b_ref)))
    ]
    for copy in copies:
        copy.start()
    for i in range(out_ref.shape[0]):
        date = first_date + i
        rest = parts_ref[2 * dates - 1 - date]
        write_unfolded(jnp.concatenate([parts_ref[date], rest[2 * SENT - SLOT :]], axis=0), out_ref.at[i])
    for copy in copies:
        copy.wait()


def unfold_pieces_kernel(parts_ref, *refs):
    *piece_refs, out_ref, packed_ref = refs
    for i in range(out_ref.shape[0]):
        packed_ref[i, 0:SENT, :] = parts_ref[i]
        for p, piece_ref in enumerate(piece_refs):
            for r in range(8):
                row = SENT + 8 * p + r
                packed_ref[i, row : row + 1, :] = piece_ref[i, :, 256 * (1 + r) : 256 * (2 + r)]
        write_unfolded(packed_ref[i], out_ref.at[i])


def write_unfolded(packed, out_ref):
    first, beside, last = unfolded(packed)
    out_ref[0:HALF, 0:HALF] = first
    out_ref[0:HALF, HALF:] = beside
    out_ref[HALF:, 0:HALF] = beside.T[0 : ROWS - HALF, :]
    out_ref[HALF:, HALF:] = last[0 : ROWS - HALF, :]


def chain_kernel(date, dates, first_date, *refs):
    inv_ref, parts_ref, phi_ref, ex_ref, m_ref, index_ref, v_ref, disc_ref = refs[:8]
    refs = refs[8:]
    if date:
        next_ref = refs[0]
        refs = refs[1:]
    if date == dates - 1:
        coefs = jnp.zeros((ROWS, 128), f32)
    else:
        coefs = refs[0][...]
        refs = refs[1:]
    if len(refs) == 4:
        refs = refs[1:]
    rhs = parts_ref[0, :, 0:256]
    for i in range(1, parts_ref.shape[0]):
        rhs = rhs + parts_ref[i, :, 0:256]
    product = inv_ref[date - first_date] * rhs
    coef = jnp.sum(product[:, 0:128] + product[:, 128:], axis=1, keepdims=True)
    coef = jnp.broadcast_to(coef, (ROWS, 128))
    out_ref, coef_ref, send_ref = refs
    continuation = []
    for c in range(0, v_ref.shape[1], 128):
        continuation.append(jnp.sum(coef * phi_ref[c // 128], axis=0, keepdims=True))
    continuation = jnp.concatenate(continuation, axis=1)
    exercise = ex_ref[date : date + 1, :]
    opened = jnp.where(index_ref[...] <= date, m_ref[date : date + 1, :].astype(f32), 0.0)
    weights = jax.nn.sigmoid((exercise - continuation) / temper_scale) * opened
    value = v_ref[...]
    value = value + weights * (exercise - value)
    if date:
        value = value * disc_ref[date - 1 : date, :]
        row = rhs_row(next_ref, value)
        for i in range(send_ref.shape[0]):
            send_ref[i, :, 0:256] = row[0:1, :]
    else:
        total = jnp.sum(value, axis=1, keepdims=True) / (value.shape[1] * parts_ref.shape[0])
        total = jnp.broadcast_to(total, (1, 128))
        for i in range(send_ref.shape[0]):
            send_ref[i] = total
    out_ref[...] = value
    coefs = jnp.where(lanes_of((ROWS, 128)) == date, coef, coefs)
    if date:
        coef_ref[...] = coefs
    else:
        for c in range(0, ROWS, 128):
            coef_ref[:, c : c + 128] = coefs[0:128, :].T if c == 0 else jnp.concatenate(
                [coefs[c:, :], jnp.zeros((128 - (ROWS - c), 128), f32)], axis=0
            ).T


def exchange(slots):
    return lax.all_to_all(slots, PATH, 0, 0, tiled=True)


def shards(states, itm_flags, terminal, strike, date_index):
    dates, factors, paths = states.shape
    size = lax.axis_size(PATH)
    sds = jax.ShapeDtypeStruct
    terminal = terminal.reshape(1, paths)
    date_index = date_index.reshape(1, paths)
    vmem = pltpu.VMEM
    limit = pltpu.CompilerParams(vmem_limit_bytes=24 << 20)
    stats = pl.pallas_call(
        stats_kernel,
        grid=(2,),
        in_specs=[
            pl.BlockSpec((dates // 2, factors, paths), lambda i: (i, 0, 0)),
            spec((dates, paths)),
        ],
        out_shape=vmem((size, 8, 128), f32),
        out_specs=WHOLE,
        scratch_shapes=[pltpu.VMEM((24, 128), f32)],
        compiler_params=limit,
        name="stats",
    )(pltpu.with_memory_space_constraint(states, pltpu.HBM), pltpu.with_memory_space_constraint(itm_flags, pltpu.HBM))
    stats = exchange(stats)
    place = jnp.full((1, 256), lax.axis_index(PATH), jnp.int32)
    exercise, discount = pl.pallas_call(
        swap_kernel,
        in_specs=[pl.BlockSpec(memory_space=pltpu.SMEM), WHOLE],
        out_specs=[WHOLE, WHOLE],
        out_shape=[vmem((dates, paths), f32), vmem((dates, paths), f32)],
        scratch_shapes=[pltpu.VMEM((factors, paths), f32)],
        compiler_params=limit,
        name="swap",
    )(strike, states)

    tiles = paths // 128
    discount, place = lax.optimization_barrier((discount, place))
    slots, value = pl.pallas_call(
        gram_kernel,
        grid=(dates,),
        in_specs=[WHOLE] * 5,
        out_specs=[WHOLE] * 2,
        out_shape=[vmem((size, SLOT, 256), f32), vmem((1, paths), f32)],
        scratch_shapes=[
            pltpu.VMEM((tiles, ROWS, 128), f32),
            pltpu.VMEM((tiles, 32, 128), f32),
            pltpu.VMEM((256, 256), f32),
            pltpu.VMEM((256, 256), f32),
            pltpu.VMEM((1, 256), f32),
            pltpu.VMEM((dates, factors, 128), f32),
            pltpu.VMEM((dates, factors, 128), f32),
        ],
        compiler_params=limit,
        name="gram",
    )(near(stats), near(states), near(itm_flags), near(discount), near(terminal))
    phi = pl.pallas_call(
        basis_kernel,
        grid=(dates,),
        in_specs=[
            spec((size, 8, 128)),
            pl.BlockSpec((None, factors, paths), lambda i: (dates - 1 - i, 0, 0)),
            spec((dates, paths)),
        ],
        out_specs=[pl.BlockSpec(memory_space=pltpu.HBM)] * dates,
        out_shape=[pltpu.HBM((tiles, ROWS, 128), f32)] * dates,
        scratch_shapes=[
            pltpu.VMEM((2, tiles, ROWS, 128), f32),
            pltpu.VMEM((tiles, 32, 128), f32),
            pltpu.SemaphoreType.DMA((2,)),
        ],
        compiler_params=limit,
        name="basis",
    )(stats, states, itm_flags)
    slots = exchange(slots)
    def invert(*refs):
        inverse_kernel(dates, *refs)

    inverse, rest, received = pl.pallas_call(
        invert,
        grid=(1,),
        in_specs=[WHOLE, WHOLE],
        out_specs=[spec((size, SENT, 256)), WHOLE, WHOLE],
        out_shape=[
            pltpu.HBM((size, SENT, 256), f32),
            vmem((SLOT - SENT, 256), f32),
            vmem((1, 1, 256), f32),
        ],
        scratch_shapes=[pltpu.VMEM((256, 256), f32)],
        compiler_params=limit,
        name="inverse",
    )(near(place), near(slots))
    inverse = exchange(inverse)
    pieces = pl.pallas_call(
        pieces_kernel,
        grid=(1,),
        in_specs=[WHOLE],
        out_specs=[spec((size, 1, WIDE))] * PIECES,
        out_shape=[pltpu.HBM((size, 1, WIDE), f32)] * PIECES,
        compiler_params=limit,
        name="pieces",
    )(near(rest))
    paired = 2 * dates - size

    def unfold_pairs(*refs):
        unfold_pairs_kernel(paired, dates, *refs)

    first_inverse, *near_phi = pl.pallas_call(
        unfold_pairs,
        grid=(1,),
        in_specs=[spec((size, SENT, 256))] + [pl.BlockSpec(memory_space=pltpu.HBM)] * 2,
        out_specs=[WHOLE] * 3,
        out_shape=[vmem((dates - paired, ROWS, 256), f32)] + [vmem((tiles, ROWS, 128), f32)] * 2,
        scratch_shapes=[pltpu.SemaphoreType.DMA((2,))],
        compiler_params=limit,
        name="unfold_pairs",
    )(inverse, *(pltpu.with_memory_space_constraint(phi[d], pltpu.HBM) for d in (dates - 1, dates - 2)))
    phi = [*phi[: dates - 2], *near_phi[::-1]]
    other_inverse = None
    carried = []
    coefs = None
    for date in range(dates - 1, -1, -1):
        if date == paired - 1:
            other_inverse = pl.pallas_call(
                unfold_pieces_kernel,
                grid=(1,),
                in_specs=[spec((paired, SENT, 256))] + [WHOLE] * PIECES,
                out_specs=WHOLE,
                out_shape=vmem((paired, ROWS, 256), f32),
                scratch_shapes=[pltpu.VMEM((paired, SLOT, 256), f32)],
                compiler_params=limit,
                name="unfold_pieces",
            )(inverse, *(near(x) for x in carried))
        first_date = paired if date >= paired else 0
        args = [first_inverse if date >= paired else other_inverse, received, phi[date], exercise, itm_flags, date_index, value, discount]
        if date:
            args.append(phi[date - 1])
        if date < dates - 1:
            args.append(coefs)
        carries = len(carried) < PIECES
        aliases = {}
        if carries:
            aliases = {len(args): 2}
            args.append(pieces[len(carried)])

        def kernel(*refs, date=date, first_date=first_date):
            chain_kernel(date, dates, first_date, *refs)

        value, coefs, send = pl.pallas_call(
            kernel,
            in_specs=[WHOLE] * len(args),
            out_specs=[WHOLE] * 3,
            out_shape=[
                vmem((1, paths), f32),
                vmem((ROWS, 128), f32),
                vmem((size, 1, WIDE if carries else 256), f32),
            ]
            if date
            else [sds((1, paths), f32), sds((128, 256), f32), sds((size, 1, 128), f32)],
            input_output_aliases=aliases,
            compiler_params=limit,
            name="chain",
        )(*(near(x) for x in args))
        received = exchange(send)
        if carries:
            carried.append(received)
    book_price = jnp.sum(received[:, 0, 0:1], axis=0)
    basis = 1 + factors + factors * (factors + 1) // 2
    coefficients = coefs[0:dates, 0:basis]
    return (value.reshape(paths), book_price, coefficients)


def solution(mesh):
    split = Mesh(mesh.devices.reshape(mesh.shape["book"], 4, 4), ("book", "path_0", "path_1"))
    return jax.shard_map(
        shards,
        mesh=split,
        in_specs=(
            P(None, None, BOOK_PATH),
            P(None, BOOK_PATH),
            P(BOOK_PATH),
            P("book"),
            P(BOOK_PATH),
        ),
        out_specs=(P(BOOK_PATH), P("book"), P("book", None)),
        check_vma=False,
    )
```

```python
import jax
import jax.numpy as jnp
from jax import lax
from jax.experimental import pallas as pl
from jax.experimental.pallas import tpu as pltpu
from jax.sharding import Mesh
from jax.sharding import PartitionSpec as P

PATH = ("path_0", "path_1")
BOOK_PATH = ("book", "path_0", "path_1")
ridge_weight = 0.05
temper_scale = 0.5
f32 = jnp.float32
bf16 = jnp.bfloat16
NT = (((1,), (1,)), ((), ()))
TN = (((0,), (0,)), ((), ()))
ROWS = 240
HALF = 128
REST = 104
SLOT = 112
SENT = 64
PIECES = 6
WIDE = 256 * 9
BLOCK = 16


def spec(shape, index=None):
    if index is None:
        index = (0,) * len(shape)
    return pl.BlockSpec(shape, lambda *_: index)


WHOLE = pl.BlockSpec(memory_space=pltpu.VMEM)


def near(x):
    return pltpu.with_memory_space_constraint(x, pltpu.VMEM)


def lanes_of(shape):
    return lax.broadcasted_iota(jnp.int32, shape, 1)


def rows_of(shape):
    return lax.broadcasted_iota(jnp.int32, shape, 0)


def stats_kernel(z_ref, m_ref, out_ref, sum_ref):
    step = pl.program_id(0)
    dates, factors, _ = z_ref.shape
    lane = lanes_of((factors, 128))

    @pl.when(step == 0)
    def _():
        sum_ref[...] = jnp.zeros_like(sum_ref)

    packed = sum_ref[0:factors, :]
    for i in range(dates):
        d = step * dates + i
        z = z_ref[i]
        m = m_ref[pl.ds(d, 1), :].astype(f32)
        mz = z * m
        packed = jnp.where(lane == 3 * d, jnp.sum(mz, axis=1, keepdims=True), packed)
        packed = jnp.where(lane == 3 * d + 1, jnp.sum(mz * z, axis=1, keepdims=True), packed)
        packed = jnp.where(lane == 3 * d + 2, jnp.sum(m, axis=1, keepdims=True), packed)
    sum_ref[0:factors, :] = packed
    groups = sum_ref[0:8] + pltpu.roll(sum_ref[8:16], 32, 1) + pltpu.roll(sum_ref[16:24], 64, 1)
    for i in range(out_ref.shape[0]):
        out_ref[i] = groups


def swap_kernel(strike_ref, z_ref, ex_ref, disc_ref, fac_ref):
    dates, factors, _ = z_ref.shape
    for d in range(dates):
        fac_ref[...] = 1.0 / (1.0 + 0.25 * (0.03 * jnp.exp(0.25 * z_ref[d])))
        first = fac_ref[0:1, :]
        disc = first
        total = first
        for j in range(1, factors):
            disc = disc * fac_ref[j : j + 1, :]
            total = total + disc
        disc_ref[d : d + 1, :] = first
        ex_ref[d : d + 1, :] = 100.0 * ((1.0 - disc) - strike_ref[0] * (0.25 * total))


def split(x):
    one = x.astype(bf16)
    rest = x - one.astype(f32)
    two = rest.astype(bf16)
    return one, two, (rest - two.astype(f32)).astype(bf16)


def rhs_row(phi_ref, weights):
    acc = jnp.zeros((ROWS, 128), f32)
    for c in range(0, weights.shape[1], 128):
        acc = acc + phi_ref[c // 128] * weights[:, c : c + 128]
    ones = jnp.ones((16, 128), bf16)
    one, two, three = (lax.dot_general(ones, x, NT, preferred_element_type=f32) for x in split(acc))
    row = (one + two + three)[0:8]
    return jnp.concatenate([row, jnp.zeros((8, 256 - ROWS), f32)], axis=1)


def column(stats, i):
    return jnp.sum(jnp.where(lanes_of(stats.shape) == i, stats, 0.0), axis=1, keepdims=True)


def moments(stats_ref, d, factors):
    stats = stats_ref[0]
    for i in range(1, stats_ref.shape[0]):
        stats = stats + stats_ref[i]
    stats = jnp.concatenate([stats, pltpu.roll(stats, 96, 1), pltpu.roll(stats, 64, 1)], axis=0)[0:factors]
    count = column(stats, 3 * d + 2)
    mean = column(stats, 3 * d) / count
    return mean, 1.0 / jnp.sqrt(column(stats, 3 * d + 1) / count - mean * mean + 1e-05)


def fill_basis(phi_ref, x_ref, z, m, mean, inverse):
    factors = z.shape[0]
    x_ref[0:factors, :] = (z - mean) * inverse * m
    phi_ref[0:1, :] = m
    phi_ref[1 : 1 + factors, :] = x_ref[0:factors, :]
    offset = 1 + factors
    for j in range(factors):
        left = jnp.broadcast_to(x_ref[j : j + 1, :], (8, 128))
        for k in range(0, factors - j, 8):
            phi_ref[offset + k : offset + k + 8, :] = left * x_ref[j + k : j + k + 8, :]
        offset += factors - j
    phi_ref[offset : offset + 8, :] = jnp.zeros((8, 128), f32)
    phi_ref[ROWS - 8 : ROWS, :] = jnp.zeros((8, 128), f32)


def basis_kernel(stats_ref, z_ref, m_ref, *refs):
    *phi_refs, phi_two_ref, x_ref, sems = refs
    step = pl.program_id(0)
    dates, paths = m_ref.shape
    d = dates - 1 - step
    side = step % 2

    def copy_of(half, date):
        return pltpu.make_async_copy(phi_two_ref.at[half], phi_refs[date], sems.at[half])

    @pl.when(step >= 2)
    def _():
        copy_of(side, 0).wait()

    mean, inverse = moments(stats_ref, d, z_ref.shape[0])
    m = m_ref[pl.ds(d, 1), :].astype(f32)
    for t in range(paths // 128):
        at = slice(t * 128, (t + 1) * 128)
        fill_basis(phi_two_ref.at[side, t], x_ref.at[t], z_ref[:, at], m[:, at], mean, inverse)
    for date in range(dates):

        @pl.when(d == date)
        def _(date=date):
            copy_of(side, date).start()

    @pl.when(step == dates - 1)
    def _():
        for half in range(2):
            copy_of(half, 0).wait()


def gram_kernel(stats_ref, z_all_ref, m_ref, disc_ref, term_ref, slots_ref, v_ref, *scratch):
    phi_ref, x_ref, gram_ref, cross_ref, rhs_ref, mean_ref, inverse_ref = scratch
    step = pl.program_id(0)
    dates, factors, paths = z_all_ref.shape
    d = dates - 1 - step

    @pl.when(step == 0)
    def _():
        x_ref[...] = jnp.zeros_like(x_ref)
        gram_ref[...] = jnp.zeros_like(gram_ref)
        cross_ref[...] = jnp.zeros_like(cross_ref)
        v_ref[...] = term_ref[...] * disc_ref[dates - 1 : dates, :]
        for date in range(dates):
            mean, inverse = moments(stats_ref, date, factors)
            mean_ref[date] = jnp.broadcast_to(mean, (factors, 128))
            inverse_ref[date] = jnp.broadcast_to(inverse, (factors, 128))

    def fold(date, first):
        cross = cross_ref[...]
        gram = gram_ref[...] + cross + cross.T
        row, lane = rows_of((HALF, HALF)), lanes_of((HALF, HALF))
        beside = jnp.where(lane < REST, gram[0:HALF, HALF:], 0.0)
        under = jnp.where((row < REST) & (lane < REST), gram[HALF:, HALF:], 0.0)
        rhs = jnp.sum(gram[ROWS : ROWS + 3, :], axis=0, keepdims=True)
        rhs = jnp.where(first, rhs, rhs_ref[...])
        rhs_ref[...] = rhs
        packed = folded(gram[0:HALF, 0:HALF], beside, under, rhs)
        slots_ref[date] = packed
        again = 2 * dates - 1 - date
        slots_ref[jnp.where(again < slots_ref.shape[0], again, date)] = packed

    fold(d + 1, step == 1)
    flags = m_ref[pl.ds(d, 1), :].astype(f32)
    values = jnp.where(step == 0, v_ref[...], 0.0)
    mean, inverse = mean_ref[d], inverse_ref[d]
    total = None
    for pair in range(0, paths // 128, 2):
        hi, lo = [], []
        for t in (pair, pair + 1):
            at = slice(t * 128, (t + 1) * 128)
            fill_basis(phi_ref.at[t], x_ref.at[t], z_all_ref[d, :, at], flags[:, at], mean, inverse)
            phi = phi_ref[t]
            high = phi.astype(bf16)
            low = (phi - high.astype(f32)).astype(bf16)
            value = values[:, at]
            one = value.astype(bf16).astype(f32)
            two = (value - one).astype(bf16).astype(f32)
            three = value - one - two
            row = rows_of((256 - ROWS, 128))
            under = jnp.where(row == 0, one, jnp.where(row == 1, two, jnp.where(row == 2, three, 0.0)))
            hi.append(jnp.concatenate([high, under.astype(bf16)], axis=0))
            lo.append(jnp.concatenate([low, jnp.zeros((256 - ROWS, 128), bf16)], axis=0))
        hi = jnp.concatenate(hi, axis=1)
        lo = jnp.concatenate(lo, axis=1)
        both = lax.dot_general(
            jnp.concatenate([hi, lo], axis=0), hi, NT, preferred_element_type=f32
        )
        total = both if total is None else total + both
    gram_ref[...] = total[0:256]
    cross_ref[...] = total[256:]

    @pl.when(step == dates - 1)
    def _():
        fold(0, False)


def folded(first, beside, last, rhs=None):
    row, lane = rows_of((HALF, HALF)), lanes_of((HALF, HALF))
    left = jnp.where(row <= lane, first, last)
    low_lane = lanes_of((8, HALF))
    low = left[REST:SLOT]
    low = jnp.where(low_lane < 16, pltpu.roll(first[SLOT : SLOT + 8], 16, 1), low)
    low = jnp.where((low_lane >= 16) & (low_lane < 32), pltpu.roll(first[SLOT + 8 :], 32, 1), low)
    if rhs is not None:
        low_row = rows_of((8, HALF))
        for i in range(4):
            piece = pltpu.roll(jnp.broadcast_to(rhs, (8, 256)), (32 - 72 * i) % 256, 1)[:, 0:HALF]
            low = jnp.where((low_row == i) & (low_lane >= 32) & (low_lane < REST), piece, low)
    left = jnp.concatenate([left[0:REST], low], axis=0)
    diagonal = jnp.sum(jnp.where(row == lane, last, 0.0), axis=1, keepdims=True)
    right = jnp.where(lane < REST, beside, pltpu.roll(beside.T, HALF - 8, 1))
    right = jnp.where(lane == 120, diagonal, right)[0:SLOT]
    return jnp.concatenate([left, right], axis=1)


def unfolded(packed):
    row, lane = rows_of((HALF, HALF)), lanes_of((HALF, HALF))
    none = jnp.zeros((HALF - SLOT, HALF), f32)
    left = jnp.concatenate([packed[:, 0:HALF], none], axis=0)
    right = jnp.concatenate([packed[:, HALF:], none], axis=0)
    low = left[REST:SLOT]
    corner = jnp.concatenate(
        [left[0:SLOT], pltpu.roll(low, HALF - 16, 1), pltpu.roll(low, HALF - 32, 1)], axis=0
    )
    turned = left.T
    first = jnp.where(row <= lane, left, turned)
    first = jnp.where((row >= SLOT) & (lane >= SLOT), corner, first)
    diagonal = jnp.sum(jnp.where(lane == 120, right, 0.0), axis=1, keepdims=True)
    last = jnp.where(row > lane, left, turned)
    last = jnp.where(row == lane, diagonal, last)
    last = jnp.where((row < REST) & (lane < REST), last, 0.0)
    beside = jnp.where(row < SLOT, right, pltpu.roll(right, 8, 1).T)
    beside = jnp.where(lane < REST, beside, 0.0)
    return first, beside, last


def unfolded_row(low):
    lane = lanes_of((1, 256))
    wide = jnp.concatenate([low, jnp.zeros((8, HALF), f32)], axis=1)
    total = jnp.zeros((1, 256), f32)
    for i in range(4):
        piece = pltpu.roll(wide, (72 * i - 32) % 256, 1)[i : i + 1]
        total = jnp.where((lane >= 72 * i) & (lane < min(72 * i + 72, 231)), piece, total)
    return total


def inverse_kernel(dates, place_ref, parts_ref, out_ref, rest_ref, rhs_ref, a_ref):
    basis = 231
    packed = parts_ref[0]
    for i in range(1, parts_ref.shape[0]):
        packed = packed + parts_ref[i]
    rhs_ref[0] = unfolded_row(packed[REST:SLOT, 0:HALF])
    first, beside, last = unfolded(packed)
    a_ref[0:HALF, 0:HALF] = first
    a_ref[0:HALF, HALF:] = beside
    a_ref[HALF:, 0:HALF] = beside.T
    a_ref[HALF:, HALF:] = last
    count = packed[0:1, 0:1]
    row, lane = rows_of((256, 256)), lanes_of((256, 256))
    added = jnp.where(row < basis, ridge_weight * count, 1.0)
    a_ref[...] = a_ref[...] + jnp.where(row == lane, added, 0.0)
    lane_a = lanes_of((8, 128))
    lane_b = lane_a + 128
    row_a = rows_of((8, 128))
    lane_r = lanes_of((BLOCK, 256))

    def sweep(i, carry):
        start = pl.multiple_of(i * BLOCK, BLOCK)
        panel = a_ref[pl.ds(start, BLOCK), :]
        halves = [[panel[g : g + 8, h : h + 128] for g in range(0, BLOCK, 8)] for h in (0, 128)]
        cols = []
        for c in range(BLOCK):
            col = []
            for g in range(BLOCK // 8):
                both = jnp.where(lane_a == start + c, halves[0][g], 0.0)
                both = both + jnp.where(lane_b == start + c, halves[1][g], 0.0)
                col.append(jnp.broadcast_to(jnp.sum(both, axis=1, keepdims=True), (8, 128)))
            cols.append(col)
        for k in range(BLOCK):
            group, at = divmod(k, 8)
            here = row_a == at
            col = cols[k]
            pivot = 1.0 / col[group][at : at + 1, :]
            unit = jnp.where(here, 1.0, 0.0)

            def reduced(groups):
                scaled = groups[group][at : at + 1, :] * pivot
                out = [x - col[g] * scaled for g, x in enumerate(groups)]
                out[group] = jnp.where(here, scaled, out[group])
                return out

            for half, lane_h in zip(halves, (lane_a, lane_b)):
                is_k = lane_h == start + k
                for g in range(BLOCK // 8):
                    half[g] = jnp.where(is_k, unit if g == group else 0.0, half[g])
                half[:] = reduced(half)
            for c in range(k + 1, BLOCK):
                cols[c] = reduced(cols[c])
        inside = (lane_r >= start) & (lane_r < start + BLOCK)
        w = jnp.concatenate([jnp.concatenate(half, axis=0) for half in halves], axis=1)
        w = jnp.where(inside, -w, w)
        r1, r2, r3 = split(panel)
        w1, w2, w3 = split(w)
        left = jnp.concatenate([r1, r1, r2, r2, r1, r3], axis=0)
        right = jnp.concatenate([w1, w2, w1, w2, w3, w1], axis=0)
        change = lax.dot_general(left, right, TN, preferred_element_type=f32)
        within = (lane >= start) & (lane < start + BLOCK)
        a_ref[...] = jnp.where(within, 0.0, a_ref[...]) - change
        a_ref[pl.ds(start, BLOCK), :] = w
        return carry

    lax.fori_loop(0, ROWS // BLOCK, sweep, 0)
    result = -a_ref[...]
    packed = folded(result[0:HALF, 0:HALF], result[0:HALF, HALF:], result[HALF:, HALF:])
    own = jnp.broadcast_to(place_ref[...] < dates, (SENT, 256))
    sent = jnp.where(own, packed[0:SENT], packed[SLOT - SENT :])
    for i in range(out_ref.shape[0]):
        out_ref[i] = sent
    rest_ref[...] = packed[SENT:SLOT]


def pieces_kernel(rest_ref, *out_refs):
    for p, out_ref in enumerate(out_refs):
        for i in range(out_ref.shape[0]):
            out_ref[i, :, 0:256] = jnp.zeros((1, 256), f32)
            for r in range(8):
                row = 8 * p + r
                out_ref[i, :, 256 * (1 + r) : 256 * (2 + r)] = rest_ref[row : row + 1, :]


def unfold_pairs_kernel(first_date, dates, far_parts_ref, *refs):
    *far_refs, out_ref, near_a_ref, near_b_ref, parts_ref, sems = refs
    own = pltpu.make_async_copy(far_parts_ref, parts_ref, sems.at[2])
    own.start()
    copies = [
        pltpu.make_async_copy(far, beside, sems.at[i])
        for i, (far, beside) in enumerate(zip(far_refs, (near_a_ref, near_b_ref)))
    ]
    for copy in copies:
        copy.start()
    own.wait()
    for i in range(out_ref.shape[0]):
        date = first_date + i
        rest = parts_ref[2 * dates - 1 - date]
        write_unfolded(jnp.concatenate([parts_ref[date], rest[2 * SENT - SLOT :]], axis=0), out_ref.at[i])
    for copy in copies:
        copy.wait()


def unfold_pieces_kernel(parts_ref, *refs):
    *piece_refs, out_ref, packed_ref = refs
    for i in range(out_ref.shape[0]):
        packed_ref[i, 0:SENT, :] = parts_ref[i]
        for p, piece_ref in enumerate(piece_refs):
            for r in range(8):
                row = SENT + 8 * p + r
                packed_ref[i, row : row + 1, :] = piece_ref[i, :, 256 * (1 + r) : 256 * (2 + r)]
        write_unfolded(packed_ref[i], out_ref.at[i])


def write_unfolded(packed, out_ref):
    first, beside, last = unfolded(packed)
    out_ref[0:HALF, 0:HALF] = first
    out_ref[0:HALF, HALF:] = beside
    out_ref[HALF:, 0:HALF] = beside.T[0 : ROWS - HALF, :]
    out_ref[HALF:, HALF:] = last[0 : ROWS - HALF, :]


def chain_kernel(date, dates, first_date, *refs):
    inv_ref, parts_ref, phi_ref, ex_ref, m_ref, index_ref, v_ref, disc_ref = refs[:8]
    refs = refs[8:]
    if date:
        next_ref = refs[0]
        refs = refs[1:]
    if date == dates - 1:
        coefs = jnp.zeros((ROWS, 128), f32)
    else:
        coefs = refs[0][...]
        refs = refs[1:]
    if len(refs) == 4:
        refs = refs[1:]
    rhs = parts_ref[0, :, 0:256]
    for i in range(1, parts_ref.shape[0]):
        rhs = rhs + parts_ref[i, :, 0:256]
    product = inv_ref[date - first_date] * rhs
    coef = jnp.sum(product[:, 0:128] + product[:, 128:], axis=1, keepdims=True)
    coef = jnp.broadcast_to(coef, (ROWS, 128))
    out_ref, coef_ref, send_ref = refs
    continuation = []
    for c in range(0, v_ref.shape[1], 128):
        continuation.append(jnp.sum(coef * phi_ref[c // 128], axis=0, keepdims=True))
    continuation = jnp.concatenate(continuation, axis=1)
    exercise = ex_ref[date : date + 1, :]
    opened = jnp.where(index_ref[...] <= date, m_ref[date : date + 1, :].astype(f32), 0.0)
    weights = jax.nn.sigmoid((exercise - continuation) / temper_scale) * opened
    value = v_ref[...]
    value = value + weights * (exercise - value)
    if date:
        value = value * disc_ref[date - 1 : date, :]
        row = rhs_row(next_ref, value)
        for i in range(send_ref.shape[0]):
            send_ref[i, :, 0:256] = row[0:1, :]
    else:
        total = jnp.sum(value, axis=1, keepdims=True) / (value.shape[1] * parts_ref.shape[0])
        total = jnp.broadcast_to(total, (1, 128))
        for i in range(send_ref.shape[0]):
            send_ref[i] = total
    out_ref[...] = value
    coefs = jnp.where(lanes_of((ROWS, 128)) == date, coef, coefs)
    if date:
        coef_ref[...] = coefs
    else:
        for c in range(0, ROWS, 128):
            coef_ref[:, c : c + 128] = coefs[0:128, :].T if c == 0 else jnp.concatenate(
                [coefs[c:, :], jnp.zeros((128 - (ROWS - c), 128), f32)], axis=0
            ).T


def exchange(slots):
    return lax.all_to_all(slots, PATH, 0, 0, tiled=True)


def shards(states, itm_flags, terminal, strike, date_index):
    dates, factors, paths = states.shape
    size = lax.axis_size(PATH)
    sds = jax.ShapeDtypeStruct
    terminal = terminal.reshape(1, paths)
    date_index = date_index.reshape(1, paths)
    vmem = pltpu.VMEM
    limit = pltpu.CompilerParams(vmem_limit_bytes=24 << 20)
    stats = pl.pallas_call(
        stats_kernel,
        grid=(2,),
        in_specs=[
            pl.BlockSpec((dates // 2, factors, paths), lambda i: (i, 0, 0)),
            spec((dates, paths)),
        ],
        out_shape=vmem((size, 8, 128), f32),
        out_specs=WHOLE,
        scratch_shapes=[pltpu.VMEM((24, 128), f32)],
        compiler_params=limit,
        name="stats",
    )(pltpu.with_memory_space_constraint(states, pltpu.HBM), pltpu.with_memory_space_constraint(itm_flags, pltpu.HBM))
    stats = exchange(stats)
    place = jnp.full((1, 256), lax.axis_index(PATH), jnp.int32)
    exercise, discount = pl.pallas_call(
        swap_kernel,
        in_specs=[pl.BlockSpec(memory_space=pltpu.SMEM), WHOLE],
        out_specs=[WHOLE, WHOLE],
        out_shape=[vmem((dates, paths), f32), vmem((dates, paths), f32)],
        scratch_shapes=[pltpu.VMEM((factors, paths), f32)],
        compiler_params=limit,
        name="swap",
    )(strike, states)

    tiles = paths // 128
    discount, place = lax.optimization_barrier((discount, place))
    slots, value = pl.pallas_call(
        gram_kernel,
        grid=(dates,),
        in_specs=[WHOLE] * 5,
        out_specs=[WHOLE] * 2,
        out_shape=[vmem((size, SLOT, 256), f32), vmem((1, paths), f32)],
        scratch_shapes=[
            pltpu.VMEM((tiles, ROWS, 128), f32),
            pltpu.VMEM((tiles, 32, 128), f32),
            pltpu.VMEM((256, 256), f32),
            pltpu.VMEM((256, 256), f32),
            pltpu.VMEM((1, 256), f32),
            pltpu.VMEM((dates, factors, 128), f32),
            pltpu.VMEM((dates, factors, 128), f32),
        ],
        compiler_params=limit,
        name="gram",
    )(near(stats), near(states), near(itm_flags), near(discount), near(terminal))
    phi = pl.pallas_call(
        basis_kernel,
        grid=(dates,),
        in_specs=[
            spec((size, 8, 128)),
            pl.BlockSpec((None, factors, paths), lambda i: (dates - 1 - i, 0, 0)),
            spec((dates, paths)),
        ],
        out_specs=[pl.BlockSpec(memory_space=pltpu.HBM)] * dates,
        out_shape=[pltpu.HBM((tiles, ROWS, 128), f32)] * dates,
        scratch_shapes=[
            pltpu.VMEM((2, tiles, ROWS, 128), f32),
            pltpu.VMEM((tiles, 32, 128), f32),
            pltpu.SemaphoreType.DMA((2,)),
        ],
        compiler_params=limit,
        name="basis",
    )(stats, states, itm_flags)
    slots = exchange(slots)
    def invert(*refs):
        inverse_kernel(dates, *refs)

    inverse, rest, received = pl.pallas_call(
        invert,
        grid=(1,),
        in_specs=[WHOLE, WHOLE],
        out_specs=[spec((size, SENT, 256)), WHOLE, WHOLE],
        out_shape=[
            pltpu.HBM((size, SENT, 256), f32),
            vmem((SLOT - SENT, 256), f32),
            vmem((1, 1, 256), f32),
        ],
        scratch_shapes=[pltpu.VMEM((256, 256), f32)],
        compiler_params=limit,
        name="inverse",
    )(near(place), near(slots))
    inverse = exchange(inverse)
    pieces = pl.pallas_call(
        pieces_kernel,
        grid=(1,),
        in_specs=[WHOLE],
        out_specs=[spec((size, 1, WIDE))] * PIECES,
        out_shape=[pltpu.HBM((size, 1, WIDE), f32)] * PIECES,
        compiler_params=limit,
        name="pieces",
    )(near(rest))
    paired = 2 * dates - size

    def unfold_pairs(*refs):
        unfold_pairs_kernel(paired, dates, *refs)

    first_inverse, *near_phi = pl.pallas_call(
        unfold_pairs,
        in_specs=[pl.BlockSpec(memory_space=pltpu.HBM)] * 3,
        out_specs=[WHOLE] * 3,
        out_shape=[vmem((dates - paired, ROWS, 256), f32)] + [vmem((tiles, ROWS, 128), f32)] * 2,
        scratch_shapes=[pltpu.VMEM((size, SENT, 256), f32), pltpu.SemaphoreType.DMA((3,))],
        compiler_params=limit,
        name="unfold_pairs",
    )(*(pltpu.with_memory_space_constraint(x, pltpu.HBM) for x in (inverse, phi[dates - 1], phi[dates - 2])))
    phi = [*phi[: dates - 2], *near_phi[::-1]]
    other_inverse = None
    carried = []
    coefs = None
    for date in range(dates - 1, -1, -1):
        if date == paired - 1:
            other_inverse = pl.pallas_call(
                unfold_pieces_kernel,
                grid=(1,),
                in_specs=[spec((paired, SENT, 256))] + [WHOLE] * PIECES,
                out_specs=WHOLE,
                out_shape=vmem((paired, ROWS, 256), f32),
                scratch_shapes=[pltpu.VMEM((paired, SLOT, 256), f32)],
                compiler_params=limit,
                name="unfold_pieces",
            )(inverse, *(near(x) for x in carried))
        first_date = paired if date >= paired else 0
        args = [first_inverse if date >= paired else other_inverse, received, phi[date], exercise, itm_flags, date_index, value, discount]
        if date:
            args.append(phi[date - 1])
        if date < dates - 1:
            args.append(coefs)
        carries = len(carried) < PIECES
        aliases = {}
        if carries:
            aliases = {len(args): 2}
            args.append(pieces[len(carried)])

        def kernel(*refs, date=date, first_date=first_date):
            chain_kernel(date, dates, first_date, *refs)

        value, coefs, send = pl.pallas_call(
            kernel,
            in_specs=[WHOLE] * len(args),
            out_specs=[WHOLE] * 3,
            out_shape=[
                vmem((1, paths), f32),
                vmem((ROWS, 128), f32),
                vmem((size, 1, WIDE if carries else 256), f32),
            ]
            if date
            else [sds((1, paths), f32), sds((128, 256), f32), sds((size, 1, 128), f32)],
            input_output_aliases=aliases,
            compiler_params=limit,
            name="chain",
        )(*(near(x) for x in args))
        received = exchange(send)
        if carries:
            carried.append(received)
    book_price = jnp.sum(received[:, 0, 0:1], axis=0)
    basis = 1 + factors + factors * (factors + 1) // 2
    coefficients = coefs[0:dates, 0:basis]
    return (value.reshape(paths), book_price, coefficients)


def solution(mesh):
    split = Mesh(mesh.devices.reshape(mesh.shape["book"], 4, 4), ("book", "path_0", "path_1"))
    return jax.shard_map(
        shards,
        mesh=split,
        in_specs=(
            P(None, None, BOOK_PATH),
            P(None, BOOK_PATH),
            P(BOOK_PATH),
            P("book"),
            P(BOOK_PATH),
        ),
        out_specs=(P(BOOK_PATH), P("book"), P("book", None)),
        check_vma=False,
    )
```
